32 devices in a mesh: row: 4 (over y, core), col: 8 (over z, x).
Axes of the slice: x: 2, y: 2, z: 4, core: 2. Of those that a mesh axis runs over, the one named last changes fastest.
Arguments:
- adjacency: int32 [8192, 8192], P('row', 'col'), may hold values from 0 to 1, as said below
Outputs:
- closure: bfloat16 [8192, 8192], P('row', 'col')
The draws below stay inside these ranges and needn't reach their ends.
Inputs may be any that keep to these rules, and one draw needn't show every extreme that they name: `adjacency`: every entry is 0 or 1; there is no bound on the number of ones in a row, a column or a block, and their share differs widely between rows and between columns.
All inputs are finite; a program needn't handle non-finite values.
Results may differ from the reference program's by a relative error of at most 0.001.
Values may be sent and summed in bfloat16 or wider, within the bound.
A program may use at most 192 MiB of HBM per device.

```python
import math
import jax
import jax.numpy as jnp
from jax import lax

PANEL = 512
PANELS = 4
ROWS = 8192
VERTS = 8192


def draw_adjacency(key, part):
    window = PANELS * PANEL
    scale_top = 1 << 20
    plain_level = scale_top // math.isqrt(window)
    sparse_level = scale_top // window
    dense_level = scale_top // 2
    key_hubs, key_levels, key_dense, key_entries = jax.random.split(jax.random.fold_in(key, 7), 4)
    hub_flags = (jax.random.randint(key_hubs, (window,), 0, 3, dtype=jnp.int32) < 2).astype(jnp.int32)
    column_hub = jnp.concatenate([hub_flags, jnp.zeros((VERTS - window,), jnp.int32)])
    row_hub = jnp.concatenate([hub_flags, jnp.zeros((ROWS - window,), jnp.int32)])
    row_ids = jnp.arange(ROWS, dtype=jnp.int32)
    levels = jax.random.randint(key_levels, (ROWS,), 0, 3, dtype=jnp.int32)
    row_plain = jnp.where(levels == 0, plain_level // 2, jnp.where(levels == 1, plain_level, plain_level * 2))
    dense_pick = jax.random.randint(key_dense, (ROWS,), 0, 16, dtype=jnp.int32)
    dense_row = (dense_pick == 0) & (row_ids >= window) | (row_hub == 1)
    on_plain = jnp.where(dense_row, dense_level, row_plain).astype(jnp.int32)
    threshold = jnp.where(column_hub[None, :] == 1, jnp.int32(sparse_level), on_plain[:, None])
    entry_draws = jax.random.randint(key_entries, (ROWS, VERTS), 0, scale_top, dtype=jnp.int32)
    return (entry_draws < threshold).astype(jnp.int32)


def setup_inputs(seed: int = 0) -> dict:
    streams_of = jax.random.split(jax.random.key(seed), 2)
    return {
        "adjacency": draw_adjacency(jax.random.fold_in(streams_of[1], 71), 0),
    }


def reference(adjacency):
    window_cols = PANELS * PANEL
    right_rows = adjacency[:window_cols].astype(jnp.float32)
    block = math.gcd(ROWS, 2048)
    blocks = adjacency.reshape(ROWS // block, block, VERTS)

    def close_rows(rows_int):
        counts = jnp.dot(rows_int[:, :window_cols].astype(jnp.float32), right_rows,
                         precision=lax.Precision.HIGHEST, preferred_element_type=jnp.float32)
        return jnp.where(counts > 0.5, 1.0, rows_int.astype(jnp.float32)).astype(jnp.bfloat16)

    return lax.map(close_rows, blocks).reshape(ROWS, VERTS)
```

```python
import functools

import jax
import jax.numpy as jnp
from jax import lax
from jax.experimental import pallas as pl
from jax.experimental.pallas import tpu as pltpu
from jax.sharding import PartitionSpec as P

PANEL = 512
PANELS = 4

CHUNK = 16
RIGHT = 128
LOAD = 256
FIRST = 64
GROUP = 256
TAIL = 128
TILE = 512
UNIT = 256
RING = 32
CREDIT = 16
PACE = RIGHT // (2 * CHUNK)
MESH = pl.DeviceIdType.MESH


def lag_of(row):
    return PACE * (1 + row) + (3 * PACE // 2) * (row // 2)


def kernel(n_rows, n_cols, window, adj_hbm, out, adj, left, right, partial,
           adj_sem, z_send, b_send, z_recv, x_send, x_recv, r_send, r_recv, credit):
    block_rows, block_cols = adj.shape
    holders = left.shape[0]
    stages = n_cols // holders
    n_chunks = block_rows // CHUNK
    n_right = window // RIGHT
    n_units = block_cols // UNIT
    per_tail = TAIL // CHUNK

    r = lax.axis_index("row")
    c = lax.axis_index("col")
    hi = c // holders
    lo = lax.rem(c, holders)
    lag = lag_of(r)

    relay = lax.rem(hi, 2) == 0
    feeds_next = relay & (hi < stages - 1)
    feeds_back = relay & (hi > 0)
    next_col = c + holders * (1 + (hi + 2 < stages).astype(jnp.int32))
    back_col = c - holders

    source = jnp.where(relay, c - 2 * holders, jnp.where(hi == stages - 1, back_col, c + holders))
    as_next = relay | (hi == stages - 1)

    def adj_copy(start, size, sem):
        rows = pl.ds(pl.multiple_of(start, CHUNK), size)
        return pltpu.make_async_copy(adj_hbm.at[rows], adj.at[rows], adj_sem.at[sem])

    def adj_load(i):
        return adj_copy(i * LOAD, LOAD, i + 1)

    head = adj_copy(0, FIRST, 0)
    neck = adj_copy(FIRST, LOAD - FIRST, 1)

    def chunk(j):
        return pl.ds(pl.multiple_of(j * CHUNK, CHUNK), CHUNK)

    def z_copy(j):
        part = left.at[lo, chunk(j)]
        return pltpu.make_async_remote_copy(
            src_ref=part, dst_ref=part, send_sem=z_send, recv_sem=z_recv.at[lax.rem(j, RING)],
            device_id={"col": next_col}, device_id_type=MESH)

    def z_back(j):
        part = left.at[lo, chunk(j)]
        return pltpu.make_async_remote_copy(
            src_ref=part, dst_ref=part, send_sem=b_send, recv_sem=z_recv.at[lax.rem(j, RING)],
            device_id={"col": back_col}, device_id_type=MESH)

    def x_copy(d, j):
        part = left.at[lo, chunk(j)]
        peer = hi * holders + lax.rem(lo + d, holders)
        return pltpu.make_async_remote_copy(
            src_ref=part, dst_ref=part, send_sem=x_send.at[d - 1], recv_sem=x_recv.at[d - 1, j // per_tail],
            device_id={"col": peer}, device_id_type=MESH)

    def x_arrival(d, i):
        part = left.at[lax.rem(lo + holders - d, holders), pl.ds(pl.multiple_of(i * TAIL, TAIL), TAIL)]
        peer = hi * holders + lax.rem(lo + holders - d, holders)
        return pltpu.make_async_remote_copy(
            src_ref=part, dst_ref=part, send_sem=x_send.at[d - 1], recv_sem=x_recv.at[d - 1, i],
            device_id={"col": peer}, device_id_type=MESH)

    def r_rows(i):
        return pl.ds(pl.multiple_of(i * RIGHT, RIGHT), RIGHT)

    def r_copy(i):
        part = right.at[r_rows(i)]
        return pltpu.make_async_remote_copy(
            src_ref=part, dst_ref=part, send_sem=r_send, recv_sem=r_recv.at[i],
            device_id={"row": r + 1}, device_id_type=MESH)

    head.start()

    barrier = pltpu.get_barrier_semaphore()

    def greet(where):
        pl.semaphore_signal(barrier, inc=1, device_id=where, device_id_type=MESH)

    @pl.when(feeds_back)
    def _():
        greet({"col": c - 2 * holders})
        greet({"col": back_col})

    @pl.when(feeds_next)
    def _():
        greet({"col": next_col})

    @pl.when(~relay & (hi < stages - 1))
    def _():
        greet({"col": c + holders})

    @pl.when(~relay & (hi == stages - 1))
    def _():
        greet({"col": c - holders})

    for d in range(1, holders):
        greet({"col": hi * holders + lax.rem(lo + d, holders)})

    @pl.when(r > 0)
    def _():
        greet({"row": r - 1})

    @pl.when(r < n_rows - 1)
    def _():
        greet({"row": r + 1})

    def convert_left(j):
        left[lo, chunk(j), :] = adj[chunk(j), :].astype(jnp.bfloat16)

    def convert_right(i):
        right[r_rows(i), :] = adj[r_rows(i), :].astype(jnp.bfloat16)

    ahead = FIRST // CHUNK
    neck.start()

    @pl.loop(1, block_rows // LOAD)
    def _(i):
        adj_load(i).start()

    head.wait()

    @pl.when(hi == 0)
    def _():
        for k in range(ahead):
            convert_left(k)

    known = (2 * feeds_back.astype(jnp.int32) + feeds_next.astype(jnp.int32)
             + (~relay).astype(jnp.int32) + (holders - 1)
             + (r > 0).astype(jnp.int32) + (r < n_rows - 1).astype(jnp.int32))
    pl.semaphore_wait(barrier, known)

    def paid(j):
        return (lax.rem(j, CREDIT) == 0) & (j >= RING)

    def pass_right(j):
        late = j - lag
        i = late // PACE

        @pl.when((late >= 0) & (lax.rem(late, PACE) == 0) & (i < n_right))
        def _():
            @pl.when(r > 0)
            def _():
                r_copy(i).wait_recv()

            @pl.when(r < n_rows - 1)
            def _():
                r_copy(i).start()

    def step(j):
        @pl.when(hi > 0)
        def _():
            z_copy(j).wait_recv()

            @pl.when((lax.rem(j + 1, CREDIT) == 0) & (j + 1 <= n_chunks - RING))
            def _():
                pl.semaphore_signal(credit.at[jnp.where(as_next, 0, 1)], inc=1,
                                    device_id={"col": source}, device_id_type=MESH)

        @pl.when(feeds_next)
        def _():
            @pl.when(paid(j))
            def _():
                pl.semaphore_wait(credit.at[0], 1)

            z_copy(j).start()

        @pl.when(feeds_back)
        def _():
            @pl.when(paid(j))
            def _():
                pl.semaphore_wait(credit.at[1], 1)

            z_back(j).start()

        for d in range(1, holders):
            x_copy(d, j).start()

        pass_right(j)

        @pl.when(j == 0)
        def _():
            neck.wait()

        per_load = 2 * PACE * LOAD // (2 * RIGHT)

        @pl.when((j > 0) & (lax.rem(j, per_load) == 0) & (j < per_load * (block_rows // LOAD)))
        def _():
            adj_load(j // per_load).wait()

        @pl.when((hi == 0) & (j + ahead < n_chunks))
        def _():
            convert_left(j + ahead)

        @pl.when((r == 0) & (lax.rem(j, PACE) == 0) & (j < PACE * n_right))
        def _():
            convert_right(j // PACE)

    def compute(u):
        g = u // n_units
        t = lax.rem(u, n_units)

        @pl.when(t == 0)
        def _():
            for d in range(1, holders):
                for k in range(GROUP // TAIL):
                    x_arrival(d, g * (GROUP // TAIL) + k).wait_recv()

        rows = pl.ds(pl.multiple_of(g * GROUP, GROUP), GROUP)
        cols = pl.ds(pl.multiple_of(t * UNIT, UNIT), UNIT)
        counts = jnp.zeros((GROUP, UNIT), jnp.float32)
        for h in range(holders):
            counts += jnp.dot(left[h, rows, :], right[h * block_cols:(h + 1) * block_cols, cols],
                              preferred_element_type=jnp.float32)
        out[rows, cols] = jnp.where(counts > 0.5, 1, adj[rows, cols]).astype(out.dtype)

    body_units = (block_rows // GROUP - 1) * n_units
    ready = PACE * (n_right - 1) + lag_of(n_rows - 1)
    first = min(n_chunks, max(ready, n_chunks - 4 - body_units))
    done = min(body_units, n_chunks - first)

    @pl.loop(0, first)
    def _(j):
        step(j)

    @pl.loop(first, n_chunks)
    def _(j):
        step(j)

        @pl.when(j - first < done)
        def _():
            compute(j - first)

    @pl.loop(n_chunks, max(n_chunks, ready + 1))
    def _(j):
        pass_right(j)

    @pl.loop(done, body_units)
    def _(u):
        compute(u)

    def arrived(start):
        for d in range(1, holders):
            x_arrival(d, start // TAIL).wait_recv()

    def half(h, start, cols):
        rights = pl.ds(pl.multiple_of(h * block_cols, block_cols), block_cols)
        return jnp.dot(left[h, start:start + TAIL, :], right[rights, cols], preferred_element_type=jnp.float32)

    tiles = [slice(t, t + TILE) for t in range(0, block_cols, TILE)]
    for start in range(block_rows - GROUP, block_rows, TAIL):
        last = start + TAIL == block_rows
        if not last:
            arrived(start)
        for cols in tiles:
            partial[:, cols] = half(lo, start, cols)
        if last:
            arrived(start)
        for cols in tiles:
            counts = partial[:, cols]
            for d in range(1, holders):
                counts += half(lax.rem(lo + holders - d, holders), start, cols)
            out[start:start + TAIL, cols] = jnp.where(
                counts > 0.5, 1, adj[start:start + TAIL, cols]).astype(out.dtype)

    whole = left.at[lo]

    @pl.when(feeds_next)
    def _():
        pltpu.make_async_remote_copy(
            src_ref=whole, dst_ref=whole, send_sem=z_send, recv_sem=z_recv.at[0],
            device_id={"col": next_col}, device_id_type=MESH).wait_send()

    @pl.when(feeds_back)
    def _():
        pltpu.make_async_remote_copy(
            src_ref=whole, dst_ref=whole, send_sem=b_send, recv_sem=z_recv.at[0],
            device_id={"col": back_col}, device_id_type=MESH).wait_send()

    for d in range(1, holders):
        pltpu.make_async_remote_copy(
            src_ref=whole, dst_ref=whole, send_sem=x_send.at[d - 1], recv_sem=x_recv.at[d - 1, 0],
            device_id={"col": hi * holders + lax.rem(lo + d, holders)}, device_id_type=MESH).wait_send()

    @pl.when(r < n_rows - 1)
    def _():
        pltpu.make_async_remote_copy(
            src_ref=right, dst_ref=right, send_sem=r_send, recv_sem=r_recv.at[0],
            device_id={"row": r + 1}, device_id_type=MESH).wait_send()


def per_device(n_rows, n_cols, adjacency):
    block_rows, block_cols = adjacency.shape
    window = PANELS * PANEL
    holders = window // block_cols
    dma = pltpu.SemaphoreType.DMA
    closed = pl.pallas_call(
        functools.partial(kernel, n_rows, n_cols, window),
        out_shape=pltpu.VMEM((block_rows, block_cols), jnp.bfloat16),
        in_specs=[pl.BlockSpec(memory_space=pltpu.HBM)],
        out_specs=pl.BlockSpec(memory_space=pltpu.VMEM),
        scratch_shapes=[
            pltpu.VMEM((block_rows, block_cols), jnp.int32),
            pltpu.VMEM((holders, block_rows, block_cols), jnp.bfloat16),
            pltpu.VMEM((window, block_cols), jnp.bfloat16),
            pltpu.VMEM((TAIL, block_cols), jnp.float32),
            dma((block_rows // LOAD + 1,)),
            dma,
            dma,
            dma((RING,)),
            dma((holders - 1,)),
            dma((holders - 1, block_rows // TAIL)),
            dma,
            dma((window // RIGHT,)),
            pltpu.SemaphoreType.REGULAR((2,)),
        ],
        compiler_params=pltpu.CompilerParams(
            collective_id=0, has_side_effects=True, vmem_limit_bytes=40 * 1024 * 1024),
    )(pltpu.with_memory_space_constraint(adjacency, pltpu.HBM))
    return closed


def solution(mesh):
    spec = P("row", "col")
    return jax.shard_map(
        functools.partial(per_device, mesh.shape["row"], mesh.shape["col"]),
        mesh=mesh, in_specs=(spec,), out_specs=spec, check_vma=False)
```

```python
import functools

import jax
import jax.numpy as jnp
from jax import lax
from jax.experimental import pallas as pl
from jax.experimental.pallas import tpu as pltpu
from jax.sharding import PartitionSpec as P

PANEL = 512
PANELS = 4

CHUNK = 8
CONVERT = 16
EVERY = CONVERT // CHUNK
FREE = 8
RIGHT = 128
LOAD = 128
FIRST = 128
GROUP = 256
TAIL = 128
SPLIT = 32
TILE = 512
UNIT = 256
RING = 32
CREDIT = 16
EARLY = ({1: 4}, {})
LATE = ({1: 4, 3: 4}, {})
PACE = RIGHT // (2 * CHUNK)
MESH = pl.DeviceIdType.MESH


def lag_of(row):
    return PACE * (1 + row) + (3 * PACE // 2) * (row // 2)


def kernel(n_rows, n_cols, window, adj_hbm, out, left, right, partial, adj,
           adj_sem, z_send, b_send, z_recv, x_send, x_recv, r_send, r_recv, credit, f_send, ready):
    block_rows, block_cols = adj.shape
    holders = left.shape[0]
    stages = n_cols // holders
    n_chunks = block_rows // CHUNK
    n_right = window // RIGHT
    n_units = block_cols // UNIT
    tail_from = n_chunks - TAIL // CHUNK
    split_from = n_chunks - SPLIT // CHUNK
    early, late = ([{stage: chunks for stage, chunks in core.items() if stage < n_cols // holders} for core in spare]
                   for spare in (EARLY, LATE))
    spared_by = [sorted({*a, *b}) for a, b in zip(early, late)]
    cores = [core for core in range(2) if spared_by[core]]

    r = lax.axis_index("row")
    c = lax.axis_index("col")
    hi = c // holders
    lo = lax.rem(c, holders)
    lag = lag_of(r)

    relay = lax.rem(hi, 2) == 0
    feeds_next = relay & (hi < stages - 1)
    feeds_back = relay & (hi > 0)
    next_col = c + holders * (1 + (hi + 2 < stages).astype(jnp.int32))
    back_col = c - holders

    source = jnp.where(relay, c - 2 * holders, jnp.where(hi == stages - 1, back_col, c + holders))
    as_next = relay | (hi == stages - 1)
    on_core = [lax.rem(r, 2) == core for core in range(2)]
    spared = [jnp.int32(0)] * 2
    for i, spare in enumerate((early, late)):
        for core in cores:
            for stage, chunks in spare[core].items():
                spared[i] = jnp.where(on_core[core] & (hi == stage), chunks, spared[i])

    def crosses(j):
        return (j < split_from - spared[0]) | ((j >= split_from) & (j < n_chunks - spared[1]))

    def load(start, size, sem):
        rows = pl.ds(pl.multiple_of(start, CONVERT), size)
        return pltpu.make_async_copy(adj_hbm.at[rows], adj.at[rows], adj_sem.at[sem])

    head = load(0, FIRST, 0)
    rest = load(FIRST, block_rows - FIRST, 1)

    def chunk(j):
        return pl.ds(pl.multiple_of(j * CHUNK, CHUNK), CHUNK)

    def z_copy(j):
        part = left.at[lo, chunk(j)]
        return pltpu.make_async_remote_copy(
            src_ref=part, dst_ref=part, send_sem=z_send, recv_sem=z_recv.at[lax.rem(j, RING)],
            device_id={"col": next_col}, device_id_type=MESH)

    def z_back(j):
        part = left.at[lo, chunk(j)]
        return pltpu.make_async_remote_copy(
            src_ref=part, dst_ref=part, send_sem=b_send, recv_sem=z_recv.at[lax.rem(j, RING)],
            device_id={"col": back_col}, device_id_type=MESH)

    def x_group(j):
        return j // (GROUP // CHUNK) + (j >= tail_from).astype(jnp.int32) + (j >= split_from).astype(jnp.int32)

    def x_copy(d, j):
        part = left.at[lo, chunk(j)]
        peer = hi * holders + lax.rem(lo + d, holders)
        return pltpu.make_async_remote_copy(
            src_ref=part, dst_ref=part, send_sem=x_send.at[d - 1], recv_sem=x_recv.at[d - 1, x_group(j)],
            device_id={"col": peer}, device_id_type=MESH)

    def x_arrival(d, group, start, size):
        part = left.at[lax.rem(lo + holders - d, holders), pl.ds(pl.multiple_of(start, CHUNK), size)]
        peer = hi * holders + lax.rem(lo + holders - d, holders)
        return pltpu.make_async_remote_copy(
            src_ref=part, dst_ref=part, send_sem=x_send.at[d - 1], recv_sem=x_recv.at[d - 1, group],
            device_id={"col": peer}, device_id_type=MESH)

    def far_copy(d, stage, chunks, end, sem):
        rows = chunks * CHUNK
        part = left.at[lax.rem(lo + holders - d, holders), pl.ds(end - rows, rows)]
        return pltpu.make_async_remote_copy(
            src_ref=part, dst_ref=part, send_sem=f_send.at[d - 1, sem],
            recv_sem=x_recv.at[d - 1, block_rows // GROUP + (end == block_rows)],
            device_id={"col": stage * holders + lo}, device_id_type=MESH)

    def far_copies(core, spare, end):
        first_sem = len(early[core]) if end == block_rows else 0
        return [far_copy(d, stage, spare[core][stage], end, first_sem + i)
                for i, stage in enumerate(sorted(spare[core], reverse=True)) for d in range(1, holders)]

    def r_rows(i):
        return pl.ds(pl.multiple_of(i * RIGHT, RIGHT), RIGHT)

    def r_copy(i):
        part = right.at[r_rows(i)]
        return pltpu.make_async_remote_copy(
            src_ref=part, dst_ref=part, send_sem=r_send, recv_sem=r_recv.at[i],
            device_id={"row": r + 1}, device_id_type=MESH)

    head.start()

    barrier = pltpu.get_barrier_semaphore()

    def greet(where):
        pl.semaphore_signal(barrier, inc=1, device_id=where, device_id_type=MESH)

    @pl.when(feeds_back)
    def _():
        greet({"col": c - 2 * holders})
        greet({"col": back_col})

    @pl.when(feeds_next)
    def _():
        greet({"col": next_col})

    @pl.when(~relay & (hi < stages - 1))
    def _():
        greet({"col": c + holders})

    @pl.when(~relay & (hi == stages - 1))
    def _():
        greet({"col": c - holders})

    for d in range(1, holders):
        greet({"col": hi * holders + lax.rem(lo + d, holders)})

    for core in cores:
        @pl.when(on_core[core] & (hi == 0))
        def _():
            for stage in spared_by[core]:
                greet({"col": stage * holders + lo})

    @pl.when(r > 0)
    def _():
        greet({"row": r - 1})

    @pl.when(r < n_rows - 1)
    def _():
        greet({"row": r + 1})

    def convert_left(i):
        rows = pl.ds(pl.multiple_of(i * CONVERT, CONVERT), CONVERT)
        left[lo, rows, :] = adj[rows, :].astype(jnp.bfloat16)

    def convert_right(i):
        right[r_rows(i), :] = adj[r_rows(i), :].astype(jnp.bfloat16)

    ahead = FIRST // CONVERT
    behind = ahead // 2

    @pl.loop(FIRST // LOAD, block_rows // LOAD)
    def _(i):
        load(i * LOAD, LOAD, 1).start()

    head.wait()

    @pl.when(hi == 0)
    def _():
        for k in range(ahead):
            convert_left(k)

    known = (2 * feeds_back.astype(jnp.int32) + feeds_next.astype(jnp.int32)
             + (~relay).astype(jnp.int32) + (holders - 1)
             + (r > 0).astype(jnp.int32) + (r < n_rows - 1).astype(jnp.int32))
    spared_here = [on_core[core] & (hi == stage) for core in cores for stage in spared_by[core]]
    for here in spared_here:
        known += here.astype(jnp.int32)
    pl.semaphore_wait(barrier, known)

    for here in spared_here:
        @pl.when(here)
        def _():
            pl.semaphore_signal(ready, inc=1, device_id={"col": lo}, device_id_type=MESH)

    def paid(j):
        return (lax.rem(j, CREDIT) == 0) & (j >= RING)

    def pass_right(j):
        late = j - lag
        i = late // PACE

        @pl.when((late >= 0) & (lax.rem(late, PACE) == 0) & (i < n_right))
        def _():
            @pl.when(r > 0)
            def _():
                r_copy(i).wait_recv()

            @pl.when(r < n_rows - 1)
            def _():
                r_copy(i).start()

    def step(j):
        @pl.when(hi > 0)
        def _():
            z_copy(j).wait_recv()

            @pl.when((lax.rem(j + 1, CREDIT) == 0) & (j + 1 <= n_chunks - RING))
            def _():
                pl.semaphore_signal(credit.at[jnp.where(as_next, 0, 1)], inc=1,
                                    device_id={"col": source}, device_id_type=MESH)

        @pl.when(feeds_next)
        def _():
            @pl.when(paid(j))
            def _():
                pl.semaphore_wait(credit.at[0], 1)

            z_copy(j).start()

        @pl.when(feeds_back)
        def _():
            @pl.when(paid(j))
            def _():
                pl.semaphore_wait(credit.at[1], 1)

            z_back(j).start()

        @pl.when(crosses(j))
        def _():
            for d in range(1, holders):
                x_copy(d, j).start()

        pass_right(j)

        @pl.when(j == EVERY * behind)
        def _():
            rest.wait()

        unit = j // EVERY + ahead - behind

        @pl.when((hi == 0) & (lax.rem(j, EVERY) == 0) & (unit >= ahead) & (unit < block_rows // CONVERT))
        def _():
            convert_left(unit)

        @pl.when((r == 0) & (lax.rem(j, PACE) == 0) & (j < PACE * n_right))
        def _():
            convert_right(j // PACE)

    def compute(u):
        g = u // n_units
        t = lax.rem(u, n_units)

        @pl.when(t == 0)
        def _():
            for d in range(1, holders):
                x_arrival(d, g, g * GROUP, GROUP).wait_recv()

        rows = pl.ds(pl.multiple_of(g * GROUP, GROUP), GROUP)
        cols = pl.ds(pl.multiple_of(t * UNIT, UNIT), UNIT)
        counts = jnp.zeros((GROUP, UNIT), jnp.float32)
        for h in range(holders):
            counts += jnp.dot(left[h, rows, :], right[h * block_cols:(h + 1) * block_cols, cols],
                              preferred_element_type=jnp.float32)
        out[rows, cols] = jnp.where(counts > 0.5, 1, adj[rows, cols]).astype(out.dtype)

    body_units = (block_rows // GROUP - 1) * n_units
    primed = PACE * (n_right - 1) + lag_of(n_rows - 1)
    gap = max(1, (n_chunks - FREE - primed) // body_units)
    first = min(n_chunks, max(primed, n_chunks - FREE - gap * body_units))
    done = min(body_units, (n_chunks - first) // gap)

    @pl.loop(0, first)
    def _(j):
        step(j)

    @pl.loop(first, n_chunks)
    def _(j):
        step(j)

        u = (j - first) // gap

        @pl.when((lax.rem(j - first, gap) == gap - 1) & (u < done))
        def _():
            compute(u)

    @pl.loop(n_chunks, max(n_chunks, primed + 1))
    def _(j):
        pass_right(j)

    @pl.loop(done, body_units)
    def _(u):
        compute(u)

    def arrived(group, start, size):
        for d in range(1, holders):
            x_arrival(d, group, start, size).wait_recv()

    def half(h, start, cols):
        rights = pl.ds(pl.multiple_of(h * block_cols, block_cols), block_cols)
        return jnp.dot(left[h, start:start + TAIL, :], right[rights, cols], preferred_element_type=jnp.float32)

    tiles = [slice(t, t + TILE) for t in range(0, block_cols, TILE)]
    start = block_rows - GROUP
    arrived(block_rows // GROUP - 1, start, TAIL)
    for cols in tiles:
        counts = half(0, start, cols)
        for h in range(1, holders):
            counts += half(h, start, cols)
        out[start:start + TAIL, cols] = jnp.where(
            counts > 0.5, 1, adj[start:start + TAIL, cols]).astype(out.dtype)

    start = block_rows - TAIL
    for cols in tiles:
        partial[:, cols] = half(lo, start, cols) + adj[start:start + TAIL, cols].astype(jnp.float32)

    arrived(block_rows // GROUP, start, TAIL - SPLIT)
    for core in cores:
        @pl.when(on_core[core] & (hi == 0))
        def _():
            pl.semaphore_wait(ready, len(spared_by[core]))
            for copy in far_copies(core, early, block_rows - SPLIT):
                copy.start()

    arrived(block_rows // GROUP + 1, block_rows - SPLIT, SPLIT)
    for core in cores:
        @pl.when(on_core[core] & (hi == 0))
        def _():
            for copy in far_copies(core, late, block_rows):
                copy.start()

    whole = left.at[lo]

    @pl.when(feeds_next)
    def _():
        pltpu.make_async_remote_copy(
            src_ref=whole, dst_ref=whole, send_sem=z_send, recv_sem=z_recv.at[0],
            device_id={"col": next_col}, device_id_type=MESH).wait_send()

    @pl.when(feeds_back)
    def _():
        pltpu.make_async_remote_copy(
            src_ref=whole, dst_ref=whole, send_sem=b_send, recv_sem=z_recv.at[0],
            device_id={"col": back_col}, device_id_type=MESH).wait_send()

    def x_sent(chunks):
        part = left.at[lo, pl.ds(0, chunks * CHUNK)]
        for d in range(1, holders):
            pltpu.make_async_remote_copy(
                src_ref=part, dst_ref=part, send_sem=x_send.at[d - 1], recv_sem=x_recv.at[d - 1, 0],
                device_id={"col": hi * holders + lax.rem(lo + d, holders)}, device_id_type=MESH).wait_send()

    for chunks in sorted({0, *(early[core].get(stage, 0) + late[core].get(stage, 0) for core in cores for stage in spared_by[core])}):
        @pl.when(spared[0] + spared[1] == chunks)
        def _():
            x_sent(n_chunks - chunks)

    for core in cores:
        @pl.when(on_core[core] & (hi == 0))
        def _():
            for copy in far_copies(core, early, block_rows - SPLIT) + far_copies(core, late, block_rows):
                copy.wait_send()

    @pl.when(r < n_rows - 1)
    def _():
        pltpu.make_async_remote_copy(
            src_ref=right, dst_ref=right, send_sem=r_send, recv_sem=r_recv.at[0],
            device_id={"row": r + 1}, device_id_type=MESH).wait_send()


def finish(closed, left, right, partial, out, tail, sems):
    holders = left.shape[0]
    block_rows, block_cols = closed.shape
    lo = lax.rem(lax.axis_index("col"), holders)
    body = block_rows - TAIL
    bulk = pltpu.make_async_copy(closed.at[0:body], out.at[0:body], sems.at[0])
    bulk.start()
    for t in range(0, block_cols, TILE):
        cols = slice(t, t + TILE)
        counts = partial[:, cols]
        for d in range(1, holders):
            h = lax.rem(lo + holders - d, holders)
            rights = pl.ds(pl.multiple_of(h * block_cols, block_cols), block_cols)
            counts += jnp.dot(left[h, body:block_rows, :], right[rights, cols], preferred_element_type=jnp.float32)
        tail[:, cols] = jnp.where(counts > 0.5, 1, 0).astype(tail.dtype)
    last = pltpu.make_async_copy(tail, out.at[body:block_rows], sems.at[1])
    last.start()
    bulk.wait()
    last.wait()


def per_device(n_rows, n_cols, adjacency):
    block_rows, block_cols = adjacency.shape
    window = PANELS * PANEL
    holders = window // block_cols
    dma = pltpu.SemaphoreType.DMA
    parts = pl.pallas_call(
        functools.partial(kernel, n_rows, n_cols, window),
        out_shape=[
            pltpu.VMEM((block_rows, block_cols), jnp.bfloat16),
            pltpu.VMEM((holders, block_rows, block_cols), jnp.bfloat16),
            pltpu.VMEM((window, block_cols), jnp.bfloat16),
            pltpu.VMEM((TAIL, block_cols), jnp.float32),
        ],
        in_specs=[pl.BlockSpec(memory_space=pltpu.HBM)],
        out_specs=[pl.BlockSpec(memory_space=pltpu.VMEM)] * 4,
        scratch_shapes=[
            pltpu.VMEM((block_rows, block_cols), jnp.int32),
            dma((2,)),
            dma,
            dma,
            dma((RING,)),
            dma((holders - 1,)),
            dma((holders - 1, block_rows // GROUP + 2)),
            dma,
            dma((window // RIGHT,)),
            pltpu.SemaphoreType.REGULAR((2,)),
            dma((holders - 1, max(len(a) + len(b) for a, b in zip(EARLY, LATE)))),
            pltpu.SemaphoreType.REGULAR,
        ],
        compiler_params=pltpu.CompilerParams(
            collective_id=0, has_side_effects=True, vmem_limit_bytes=20 * 1024 * 1024),
    )(pltpu.with_memory_space_constraint(adjacency, pltpu.HBM))
    return pl.pallas_call(
        finish,
        out_shape=jax.ShapeDtypeStruct((block_rows, block_cols), jnp.bfloat16),
        in_specs=[pl.BlockSpec(memory_space=pltpu.VMEM)] * 4,
        out_specs=pl.BlockSpec(memory_space=pltpu.HBM),
        scratch_shapes=[pltpu.VMEM((TAIL, block_cols), jnp.bfloat16), dma((2,))],
        compiler_params=pltpu.CompilerParams(vmem_limit_bytes=8 * 1024 * 1024),
    )(*parts)


def solution(mesh):
    spec = P("row", "col")
    return jax.shard_map(
        functools.partial(per_device, mesh.shape["row"], mesh.shape["col"]),
        mesh=mesh, in_specs=(spec,), out_specs=spec, check_vma=False)
```

```python
import functools

import jax
import jax.numpy as jnp
from jax import lax
from jax.experimental import pallas as pl
from jax.experimental.pallas import tpu as pltpu
from jax.sharding import PartitionSpec as P

PANEL = 512
PANELS = 4

CHUNK = 8
CONVERT = 16
EVERY = CONVERT // CHUNK
FREE = 8
RIGHT = 128
LOAD = 128
FIRST = 128
GROUP = 256
TAIL = 128
SPLIT = 32
TILE = 512
UNIT = 256
RING = 32
CREDIT = 16
RIGHTS = 4
EARLY = ({1: 5}, {})
LATE = ({1: 4, 3: 4}, {1: 2})
PACE = RIGHT // (2 * CHUNK)
MESH = pl.DeviceIdType.MESH


def lag_of(row):
    return PACE * (1 + row) + (3 * PACE // 2) * (row // 2)


def kernel(n_rows, n_cols, window, adj_hbm, out, left, right, partial, adj,
           adj_sem, z_send, b_send, z_recv, x_send, x_recv, r_send, r_recv, credit, f_send, ready):
    block_rows, block_cols = adj.shape
    holders = left.shape[0]
    stages = n_cols // holders
    n_chunks = block_rows // CHUNK
    n_right = window // RIGHT
    n_units = block_cols // UNIT
    tail_from = n_chunks - TAIL // CHUNK
    split_from = n_chunks - SPLIT // CHUNK
    early, late = ([{stage: chunks for stage, chunks in core.items() if stage < n_cols // holders} for core in spare]
                   for spare in (EARLY, LATE))
    spared_by = [sorted({*a, *b}) for a, b in zip(early, late)]
    cores = [core for core in range(2) if spared_by[core]]

    r = lax.axis_index("row")
    c = lax.axis_index("col")
    hi = c // holders
    lo = lax.rem(c, holders)
    lag = lag_of(r)

    relay = lax.rem(hi, 2) == 0
    feeds_next = relay & (hi < stages - 1)
    feeds_back = relay & (hi > 0)
    next_col = c + holders * (1 + (hi + 2 < stages).astype(jnp.int32))
    back_col = c - holders

    source = jnp.where(relay, c - 2 * holders, jnp.where(hi == stages - 1, back_col, c + holders))
    as_next = relay | (hi == stages - 1)
    on_core = [lax.rem(r, 2) == core for core in range(2)]
    spared = [jnp.int32(0)] * 2
    for i, spare in enumerate((early, late)):
        for core in cores:
            for stage, chunks in spare[core].items():
                spared[i] = jnp.where(on_core[core] & (hi == stage), chunks, spared[i])

    def crosses(j):
        return (j < split_from - spared[0]) | ((j >= split_from) & (j < n_chunks - spared[1]))

    def load(start, size, sem):
        rows = pl.ds(pl.multiple_of(start, CONVERT), size)
        return pltpu.make_async_copy(adj_hbm.at[rows], adj.at[rows], adj_sem.at[sem])

    head = load(0, FIRST, 0)
    rest = load(FIRST, block_rows - FIRST, 1)

    def chunk(j):
        return pl.ds(pl.multiple_of(j * CHUNK, CHUNK), CHUNK)

    def z_copy(j):
        part = left.at[lo, chunk(j)]
        return pltpu.make_async_remote_copy(
            src_ref=part, dst_ref=part, send_sem=z_send, recv_sem=z_recv.at[lax.rem(j, RING)],
            device_id={"col": next_col}, device_id_type=MESH)

    def z_back(j):
        part = left.at[lo, chunk(j)]
        return pltpu.make_async_remote_copy(
            src_ref=part, dst_ref=part, send_sem=b_send, recv_sem=z_recv.at[lax.rem(j, RING)],
            device_id={"col": back_col}, device_id_type=MESH)

    def x_group(j):
        return j // (GROUP // CHUNK) + (j >= tail_from).astype(jnp.int32) + (j >= split_from).astype(jnp.int32)

    def x_copy(d, j):
        part = left.at[lo, chunk(j)]
        peer = hi * holders + lax.rem(lo + d, holders)
        return pltpu.make_async_remote_copy(
            src_ref=part, dst_ref=part, send_sem=x_send.at[d - 1], recv_sem=x_recv.at[d - 1, x_group(j)],
            device_id={"col": peer}, device_id_type=MESH)

    def x_arrival(d, group, start, size):
        part = left.at[lax.rem(lo + holders - d, holders), pl.ds(pl.multiple_of(start, CHUNK), size)]
        peer = hi * holders + lax.rem(lo + holders - d, holders)
        return pltpu.make_async_remote_copy(
            src_ref=part, dst_ref=part, send_sem=x_send.at[d - 1], recv_sem=x_recv.at[d - 1, group],
            device_id={"col": peer}, device_id_type=MESH)

    def far_copy(d, stage, chunks, end, sem):
        rows = chunks * CHUNK
        part = left.at[lax.rem(lo + holders - d, holders), pl.ds(end - rows, rows)]
        return pltpu.make_async_remote_copy(
            src_ref=part, dst_ref=part, send_sem=f_send.at[d - 1, sem],
            recv_sem=x_recv.at[d - 1, block_rows // GROUP + (end == block_rows)],
            device_id={"col": stage * holders + lo}, device_id_type=MESH)

    def far_copies(core, spare, end):
        first_sem = len(early[core]) if end == block_rows else 0
        return [far_copy(d, stage, spare[core][stage], end, first_sem + i)
                for i, stage in enumerate(sorted(spare[core], reverse=True)) for d in range(1, holders)]

    def r_rows(i):
        return pl.ds(pl.multiple_of(i * RIGHT, RIGHT), RIGHT)

    def r_copy(i):
        part = right.at[r_rows(i)]
        return pltpu.make_async_remote_copy(
            src_ref=part, dst_ref=part, send_sem=r_send, recv_sem=r_recv.at[lax.rem(i, RIGHTS)],
            device_id={"row": r + 1}, device_id_type=MESH)

    head.start()

    barrier = pltpu.get_barrier_semaphore()

    def greet(where):
        pl.semaphore_signal(barrier, inc=1, device_id=where, device_id_type=MESH)

    @pl.when(feeds_back)
    def _():
        greet({"col": c - 2 * holders})
        greet({"col": back_col})

    @pl.when(feeds_next)
    def _():
        greet({"col": next_col})

    @pl.when(~relay & (hi < stages - 1))
    def _():
        greet({"col": c + holders})

    @pl.when(~relay & (hi == stages - 1))
    def _():
        greet({"col": c - holders})

    for d in range(1, holders):
        greet({"col": hi * holders + lax.rem(lo + d, holders)})

    for core in cores:
        @pl.when(on_core[core] & (hi == 0))
        def _():
            for stage in spared_by[core]:
                greet({"col": stage * holders + lo})

    @pl.when(r > 0)
    def _():
        greet({"row": r - 1})

    @pl.when(r < n_rows - 1)
    def _():
        greet({"row": r + 1})

    def convert_left(i):
        rows = pl.ds(pl.multiple_of(i * CONVERT, CONVERT), CONVERT)
        left[lo, rows, :] = adj[rows, :].astype(jnp.bfloat16)

    def convert_right(i):
        right[r_rows(i), :] = adj[r_rows(i), :].astype(jnp.bfloat16)

    ahead = FIRST // CONVERT
    behind = ahead // 2

    @pl.loop(FIRST // LOAD, block_rows // LOAD)
    def _(i):
        load(i * LOAD, LOAD, 1).start()

    head.wait()

    @pl.when(hi == 0)
    def _():
        for k in range(ahead):
            convert_left(k)

    known = (2 * feeds_back.astype(jnp.int32) + feeds_next.astype(jnp.int32)
             + (~relay).astype(jnp.int32) + (holders - 1)
             + (r > 0).astype(jnp.int32) + (r < n_rows - 1).astype(jnp.int32))
    spared_here = [on_core[core] & (hi == stage) for core in cores for stage in spared_by[core]]
    for here in spared_here:
        known += here.astype(jnp.int32)
    pl.semaphore_wait(barrier, known)

    for here in spared_here:
        @pl.when(here)
        def _():
            pl.semaphore_signal(ready, inc=1, device_id={"col": lo}, device_id_type=MESH)

    def paid(j):
        return (lax.rem(j, CREDIT) == 0) & (j >= RING)

    def pass_right(j):
        late = j - lag
        i = late // PACE

        @pl.when((late >= 0) & (lax.rem(late, PACE) == 0) & (i < n_right))
        def _():
            @pl.when(r > 0)
            def _():
                r_copy(i).wait_recv()

                @pl.when(i < n_right - RIGHTS)
                def _():
                    pl.semaphore_signal(credit.at[2], inc=1, device_id={"row": r - 1}, device_id_type=MESH)

            @pl.when(r < n_rows - 1)
            def _():
                @pl.when(i >= RIGHTS)
                def _():
                    pl.semaphore_wait(credit.at[2], 1)

                r_copy(i).start()

    def step(j):
        @pl.when(hi > 0)
        def _():
            z_copy(j).wait_recv()

        @pl.when(feeds_next)
        def _():
            @pl.when(paid(j))
            def _():
                pl.semaphore_wait(credit.at[0], 1)

            z_copy(j).start()

        @pl.when(feeds_back)
        def _():
            @pl.when(paid(j))
            def _():
                pl.semaphore_wait(credit.at[1], 1)

            z_back(j).start()

        @pl.when(crosses(j))
        def _():
            for d in range(1, holders):
                x_copy(d, j).start()

        @pl.when((hi > 0) & (lax.rem(j + 1, CREDIT) == 0) & (j + 1 <= n_chunks - RING))
        def _():
            pl.semaphore_signal(credit.at[jnp.where(as_next, 0, 1)], inc=1,
                                device_id={"col": source}, device_id_type=MESH)

        pass_right(j)

        @pl.when(j == EVERY * behind)
        def _():
            rest.wait()

        unit = j // EVERY + ahead - behind

        @pl.when((hi == 0) & (lax.rem(j, EVERY) == 0) & (unit >= ahead) & (unit < block_rows // CONVERT))
        def _():
            convert_left(unit)

        @pl.when((r == 0) & (lax.rem(j, PACE) == 0) & (j < PACE * n_right))
        def _():
            convert_right(j // PACE)

    def compute(u):
        g = u // n_units
        t = lax.rem(u, n_units)

        @pl.when(t == 0)
        def _():
            for d in range(1, holders):
                x_arrival(d, g, g * GROUP, GROUP).wait_recv()

        rows = pl.ds(pl.multiple_of(g * GROUP, GROUP), GROUP)
        cols = pl.ds(pl.multiple_of(t * UNIT, UNIT), UNIT)
        counts = jnp.zeros((GROUP, UNIT), jnp.float32)
        for h in range(holders):
            counts += jnp.dot(left[h, rows, :], right[h * block_cols:(h + 1) * block_cols, cols],
                              preferred_element_type=jnp.float32)
        out[rows, cols] = jnp.where(counts > 0.5, 1, adj[rows, cols]).astype(out.dtype)

    body_units = (block_rows // GROUP - 1) * n_units
    primed = PACE * (n_right - 1) + lag_of(n_rows - 1)
    gap = max(1, (n_chunks - FREE - primed) // body_units)
    first = min(n_chunks, max(primed, n_chunks - FREE - gap * body_units))
    done = min(body_units, (n_chunks - first) // gap)

    @pl.loop(0, first)
    def _(j):
        step(j)

    @pl.loop(first, n_chunks)
    def _(j):
        step(j)

        u = (j - first) // gap

        @pl.when((lax.rem(j - first, gap) == gap - 1) & (u < done))
        def _():
            compute(u)

    @pl.loop(n_chunks, max(n_chunks, primed + 1))
    def _(j):
        pass_right(j)

    @pl.loop(done, body_units)
    def _(u):
        compute(u)

    def arrived(group, start, size):
        for d in range(1, holders):
            x_arrival(d, group, start, size).wait_recv()

    def half(h, start, cols):
        rights = pl.ds(pl.multiple_of(h * block_cols, block_cols), block_cols)
        return jnp.dot(left[h, start:start + TAIL, :], right[rights, cols], preferred_element_type=jnp.float32)

    tiles = [slice(t, t + TILE) for t in range(0, block_cols, TILE)]
    start = block_rows - GROUP
    arrived(block_rows // GROUP - 1, start, TAIL)
    for cols in tiles:
        counts = half(0, start, cols)
        for h in range(1, holders):
            counts += half(h, start, cols)
        out[start:start + TAIL, cols] = jnp.where(
            counts > 0.5, 1, adj[start:start + TAIL, cols]).astype(out.dtype)

    start = block_rows - TAIL
    for cols in tiles:
        partial[:, cols] = half(lo, start, cols) + adj[start:start + TAIL, cols].astype(jnp.float32)

    arrived(block_rows // GROUP, start, TAIL - SPLIT)
    for core in cores:
        @pl.when(on_core[core] & (hi == 0))
        def _():
            pl.semaphore_wait(ready, len(spared_by[core]))
            for copy in far_copies(core, early, block_rows - SPLIT):
                copy.start()

    arrived(block_rows // GROUP + 1, block_rows - SPLIT, SPLIT)
    for core in cores:
        @pl.when(on_core[core] & (hi == 0))
        def _():
            for copy in far_copies(core, late, block_rows):
                copy.start()

    whole = left.at[lo]

    @pl.when(feeds_next)
    def _():
        pltpu.make_async_remote_copy(
            src_ref=whole, dst_ref=whole, send_sem=z_send, recv_sem=z_recv.at[0],
            device_id={"col": next_col}, device_id_type=MESH).wait_send()

    @pl.when(feeds_back)
    def _():
        pltpu.make_async_remote_copy(
            src_ref=whole, dst_ref=whole, send_sem=b_send, recv_sem=z_recv.at[0],
            device_id={"col": back_col}, device_id_type=MESH).wait_send()

    def x_sent(chunks):
        part = left.at[lo, pl.ds(0, chunks * CHUNK)]
        for d in range(1, holders):
            pltpu.make_async_remote_copy(
                src_ref=part, dst_ref=part, send_sem=x_send.at[d - 1], recv_sem=x_recv.at[d - 1, 0],
                device_id={"col": hi * holders + lax.rem(lo + d, holders)}, device_id_type=MESH).wait_send()

    for chunks in sorted({0, *(early[core].get(stage, 0) + late[core].get(stage, 0) for core in cores for stage in spared_by[core])}):
        @pl.when(spared[0] + spared[1] == chunks)
        def _():
            x_sent(n_chunks - chunks)

    for core in cores:
        @pl.when(on_core[core] & (hi == 0))
        def _():
            for copy in far_copies(core, early, block_rows - SPLIT) + far_copies(core, late, block_rows):
                copy.wait_send()

    @pl.when(r < n_rows - 1)
    def _():
        pltpu.make_async_remote_copy(
            src_ref=right, dst_ref=right, send_sem=r_send, recv_sem=r_recv.at[0],
            device_id={"row": r + 1}, device_id_type=MESH).wait_send()


def finish(closed, left, right, partial, out, tail, sems):
    holders = left.shape[0]
    block_rows, block_cols = closed.shape
    lo = lax.rem(lax.axis_index("col"), holders)
    body = block_rows - TAIL
    bulk = pltpu.make_async_copy(closed.at[0:body], out.at[0:body], sems.at[0])
    bulk.start()
    for t in range(0, block_cols, TILE):
        cols = slice(t, t + TILE)
        counts = partial[:, cols]
        for d in range(1, holders):
            h = lax.rem(lo + holders - d, holders)
            rights = pl.ds(pl.multiple_of(h * block_cols, block_cols), block_cols)
            counts += jnp.dot(left[h, body:block_rows, :], right[rights, cols], preferred_element_type=jnp.float32)
        tail[:, cols] = jnp.where(counts > 0.5, 1, 0).astype(tail.dtype)
    last = pltpu.make_async_copy(tail, out.at[body:block_rows], sems.at[1])
    last.start()
    bulk.wait()
    last.wait()


def per_device(n_rows, n_cols, adjacency):
    block_rows, block_cols = adjacency.shape
    window = PANELS * PANEL
    holders = window // block_cols
    dma = pltpu.SemaphoreType.DMA
    parts = pl.pallas_call(
        functools.partial(kernel, n_rows, n_cols, window),
        out_shape=[
            pltpu.VMEM((block_rows, block_cols), jnp.bfloat16),
            pltpu.VMEM((holders, block_rows, block_cols), jnp.bfloat16),
            pltpu.VMEM((window, block_cols), jnp.bfloat16),
            pltpu.VMEM((TAIL, block_cols), jnp.float32),
        ],
        in_specs=[pl.BlockSpec(memory_space=pltpu.HBM)],
        out_specs=[pl.BlockSpec(memory_space=pltpu.VMEM)] * 4,
        scratch_shapes=[
            pltpu.VMEM((block_rows, block_cols), jnp.int32),
            dma((2,)),
            dma,
            dma,
            dma((RING,)),
            dma((holders - 1,)),
            dma((holders - 1, block_rows // GROUP + 2)),
            dma,
            dma((RIGHTS,)),
            pltpu.SemaphoreType.REGULAR((3,)),
            dma((holders - 1, max(len(a) + len(b) for a, b in zip(EARLY, LATE)))),
            pltpu.SemaphoreType.REGULAR,
        ],
        compiler_params=pltpu.CompilerParams(
            collective_id=0, has_side_effects=True, vmem_limit_bytes=20 * 1024 * 1024),
    )(pltpu.with_memory_space_constraint(adjacency, pltpu.HBM))
    return pl.pallas_call(
        finish,
        out_shape=jax.ShapeDtypeStruct((block_rows, block_cols), jnp.bfloat16),
        in_specs=[pl.BlockSpec(memory_space=pltpu.VMEM)] * 4,
        out_specs=pl.BlockSpec(memory_space=pltpu.HBM),
        scratch_shapes=[pltpu.VMEM((TAIL, block_cols), jnp.bfloat16), dma((2,))],
        compiler_params=pltpu.CompilerParams(vmem_limit_bytes=8 * 1024 * 1024),
    )(*parts)


def solution(mesh):
    spec = P("row", "col")
    return jax.shard_map(
        functools.partial(per_device, mesh.shape["row"], mesh.shape["col"]),
        mesh=mesh, in_specs=(spec,), out_specs=spec, check_vma=False)
```

```python
import functools

import jax
import jax.numpy as jnp
from jax import lax
from jax.experimental import pallas as pl
from jax.experimental.pallas import tpu as pltpu
from jax.sharding import PartitionSpec as P

PANEL = 512
PANELS = 4

CHUNK = 8
CONVERT = 16
EVERY = CONVERT // CHUNK
FREE = 8
RIGHT = 128
LOAD = 128
FIRST = 128
GROUP = 256
PAIR = 2 * GROUP // CHUNK
TAIL = 128
SPLIT = 32
TILE = 512
UNIT = 256
RING = 32
CREDIT = 16
RIGHTS = 4
EARLY = ({1: 5}, {})
LATE = ({1: 4, 3: 4}, {1: 2})
PACE = RIGHT // (2 * CHUNK)
MESH = pl.DeviceIdType.MESH


def lag_of(row):
    return PACE * (1 + row) + (3 * PACE // 2) * (row // 2)


def kernel(n_rows, n_cols, window, adj_hbm, out, left, right, partial, adj,
           adj_sem, z_send, b_send, z_recv, x_send, x_recv, r_send, r_recv, credit, f_send, ready):
    block_rows, block_cols = adj.shape
    holders = left.shape[0]
    stages = n_cols // holders
    n_chunks = block_rows // CHUNK
    n_right = window // RIGHT
    n_units = block_cols // UNIT
    tail_from = n_chunks - TAIL // CHUNK
    split_from = n_chunks - SPLIT // CHUNK
    paired = (block_rows // GROUP - 1) // 2
    tail_sem = block_rows // GROUP - paired - 1
    early, late = ([{stage: chunks for stage, chunks in core.items() if stage < n_cols // holders} for core in spare]
                   for spare in (EARLY, LATE))
    spared_by = [sorted({*a, *b}) for a, b in zip(early, late)]
    cores = [core for core in range(2) if spared_by[core]]

    r = lax.axis_index("row")
    c = lax.axis_index("col")
    hi = c // holders
    lo = lax.rem(c, holders)
    lag = lag_of(r)

    relay = lax.rem(hi, 2) == 0
    feeds_next = relay & (hi < stages - 1)
    feeds_back = relay & (hi > 0)
    next_col = c + holders * (1 + (hi + 2 < stages).astype(jnp.int32))
    back_col = c - holders

    source = jnp.where(relay, c - 2 * holders, jnp.where(hi == stages - 1, back_col, c + holders))
    as_next = relay | (hi == stages - 1)
    on_core = [lax.rem(r, 2) == core for core in range(2)]
    spared = [jnp.int32(0)] * 2
    for i, spare in enumerate((early, late)):
        for core in cores:
            for stage, chunks in spare[core].items():
                spared[i] = jnp.where(on_core[core] & (hi == stage), chunks, spared[i])

    def crosses(j):
        return (j < split_from - spared[0]) | ((j >= split_from) & (j < n_chunks - spared[1]))

    def load(start, size, sem):
        rows = pl.ds(pl.multiple_of(start, CONVERT), size)
        return pltpu.make_async_copy(adj_hbm.at[rows], adj.at[rows], adj_sem.at[sem])

    head = load(0, FIRST, 0)
    rest = load(FIRST, block_rows - FIRST, 1)

    def chunk(j):
        return pl.ds(pl.multiple_of(j * CHUNK, CHUNK), CHUNK)

    def z_copy(j):
        part = left.at[lo, chunk(j)]
        return pltpu.make_async_remote_copy(
            src_ref=part, dst_ref=part, send_sem=z_send, recv_sem=z_recv.at[lax.rem(j, RING)],
            device_id={"col": next_col}, device_id_type=MESH)

    def z_back(j):
        part = left.at[lo, chunk(j)]
        return pltpu.make_async_remote_copy(
            src_ref=part, dst_ref=part, send_sem=b_send, recv_sem=z_recv.at[lax.rem(j, RING)],
            device_id={"col": back_col}, device_id_type=MESH)

    def x_group(j):
        return jnp.minimum(j // PAIR, paired) + jnp.maximum(j // (GROUP // CHUNK) - 2 * paired, 0) + (j >= tail_from).astype(jnp.int32) + (j >= split_from).astype(jnp.int32)

    def x_copy(d, j):
        part = left.at[lo, chunk(j)]
        peer = hi * holders + lax.rem(lo + d, holders)
        return pltpu.make_async_remote_copy(
            src_ref=part, dst_ref=part, send_sem=x_send.at[d - 1], recv_sem=x_recv.at[d - 1, x_group(j)],
            device_id={"col": peer}, device_id_type=MESH)

    def x_arrival(d, group, start, size):
        part = left.at[lax.rem(lo + holders - d, holders), pl.ds(pl.multiple_of(start, CHUNK), size)]
        peer = hi * holders + lax.rem(lo + holders - d, holders)
        return pltpu.make_async_remote_copy(
            src_ref=part, dst_ref=part, send_sem=x_send.at[d - 1], recv_sem=x_recv.at[d - 1, group],
            device_id={"col": peer}, device_id_type=MESH)

    def far_copy(d, stage, chunks, end, sem):
        rows = chunks * CHUNK
        part = left.at[lax.rem(lo + holders - d, holders), pl.ds(end - rows, rows)]
        return pltpu.make_async_remote_copy(
            src_ref=part, dst_ref=part, send_sem=f_send.at[d - 1, sem],
            recv_sem=x_recv.at[d - 1, tail_sem + 1 + (end == block_rows)],
            device_id={"col": stage * holders + lo}, device_id_type=MESH)

    def far_copies(core, spare, end):
        first_sem = len(early[core]) if end == block_rows else 0
        return [far_copy(d, stage, spare[core][stage], end, first_sem + i)
                for i, stage in enumerate(sorted(spare[core], reverse=True)) for d in range(1, holders)]

    def r_rows(i):
        return pl.ds(pl.multiple_of(i * RIGHT, RIGHT), RIGHT)

    def r_copy(i):
        part = right.at[r_rows(i)]
        return pltpu.make_async_remote_copy(
            src_ref=part, dst_ref=part, send_sem=r_send, recv_sem=r_recv.at[lax.rem(i, RIGHTS)],
            device_id={"row": r + 1}, device_id_type=MESH)

    head.start()

    barrier = pltpu.get_barrier_semaphore()

    def greet(where):
        pl.semaphore_signal(barrier, inc=1, device_id=where, device_id_type=MESH)

    @pl.when(feeds_back)
    def _():
        greet({"col": c - 2 * holders})
        greet({"col": back_col})

    @pl.when(feeds_next)
    def _():
        greet({"col": next_col})

    @pl.when(~relay & (hi < stages - 1))
    def _():
        greet({"col": c + holders})

    @pl.when(~relay & (hi == stages - 1))
    def _():
        greet({"col": c - holders})

    for d in range(1, holders):
        greet({"col": hi * holders + lax.rem(lo + d, holders)})

    for core in cores:
        @pl.when(on_core[core] & (hi == 0))
        def _():
            for stage in spared_by[core]:
                greet({"col": stage * holders + lo})

    @pl.when(r > 0)
    def _():
        greet({"row": r - 1})

    @pl.when(r < n_rows - 1)
    def _():
        greet({"row": r + 1})

    def convert_left(i):
        rows = pl.ds(pl.multiple_of(i * CONVERT, CONVERT), CONVERT)
        left[lo, rows, :] = adj[rows, :].astype(jnp.bfloat16)

    def convert_right(i):
        right[r_rows(i), :] = adj[r_rows(i), :].astype(jnp.bfloat16)

    ahead = FIRST // CONVERT
    behind = ahead // 2

    @pl.loop(FIRST // LOAD, block_rows // LOAD)
    def _(i):
        load(i * LOAD, LOAD, 1).start()

    head.wait()

    @pl.when(hi == 0)
    def _():
        for k in range(ahead):
            convert_left(k)

    known = (2 * feeds_back.astype(jnp.int32) + feeds_next.astype(jnp.int32)
             + (~relay).astype(jnp.int32) + (holders - 1)
             + (r > 0).astype(jnp.int32) + (r < n_rows - 1).astype(jnp.int32))
    spared_here = [on_core[core] & (hi == stage) for core in cores for stage in spared_by[core]]
    for here in spared_here:
        known += here.astype(jnp.int32)
    pl.semaphore_wait(barrier, known)

    for here in spared_here:
        @pl.when(here)
        def _():
            pl.semaphore_signal(ready, inc=1, device_id={"col": lo}, device_id_type=MESH)

    def paid(j):
        return (lax.rem(j, CREDIT) == 0) & (j >= RING)

    def pass_right(j):
        late = j - lag
        i = late // PACE

        @pl.when((late >= 0) & (lax.rem(late, PACE) == 0) & (i < n_right))
        def _():
            @pl.when(r > 0)
            def _():
                r_copy(i).wait_recv()

                @pl.when(i < n_right - RIGHTS)
                def _():
                    pl.semaphore_signal(credit.at[2], inc=1, device_id={"row": r - 1}, device_id_type=MESH)

            @pl.when(r < n_rows - 1)
            def _():
                @pl.when(i >= RIGHTS)
                def _():
                    pl.semaphore_wait(credit.at[2], 1)

                r_copy(i).start()

    def step(j):
        @pl.when(hi > 0)
        def _():
            z_copy(j).wait_recv()

        @pl.when(feeds_next)
        def _():
            @pl.when(paid(j))
            def _():
                pl.semaphore_wait(credit.at[0], 1)

            z_copy(j).start()

        @pl.when(feeds_back)
        def _():
            @pl.when(paid(j))
            def _():
                pl.semaphore_wait(credit.at[1], 1)

            z_back(j).start()

        @pl.when(crosses(j))
        def _():
            for d in range(1, holders):
                x_copy(d, j).start()

        @pl.when((hi > 0) & (lax.rem(j + 1, CREDIT) == 0) & (j + 1 <= n_chunks - RING))
        def _():
            pl.semaphore_signal(credit.at[jnp.where(as_next, 0, 1)], inc=1,
                                device_id={"col": source}, device_id_type=MESH)

        pass_right(j)

        @pl.when(j == EVERY * behind)
        def _():
            rest.wait()

        unit = j // EVERY + ahead - behind

        @pl.when((hi == 0) & (lax.rem(j, EVERY) == 0) & (unit >= ahead) & (unit < block_rows // CONVERT))
        def _():
            convert_left(unit)

        @pl.when((r == 0) & (lax.rem(j, PACE) == 0) & (j < PACE * n_right))
        def _():
            convert_right(j // PACE)

    def compute(u):
        g = u // n_units
        t = lax.rem(u, n_units)

        @pl.when((t == 0) & (lax.rem(g, 2) == 0) & (g < 2 * paired))
        def _():
            for d in range(1, holders):
                x_arrival(d, g // 2, g * GROUP, 2 * GROUP).wait_recv()

        @pl.when((t == 0) & (g >= 2 * paired))
        def _():
            for d in range(1, holders):
                x_arrival(d, g - paired, g * GROUP, GROUP).wait_recv()

        rows = pl.ds(pl.multiple_of(g * GROUP, GROUP), GROUP)
        cols = pl.ds(pl.multiple_of(t * UNIT, UNIT), UNIT)
        counts = jnp.zeros((GROUP, UNIT), jnp.float32)
        for h in range(holders):
            counts += jnp.dot(left[h, rows, :], right[h * block_cols:(h + 1) * block_cols, cols],
                              preferred_element_type=jnp.float32)
        out[rows, cols] = jnp.where(counts > 0.5, 1, adj[rows, cols]).astype(out.dtype)

    body_units = (block_rows // GROUP - 1) * n_units
    primed = PACE * (n_right - 1) + lag_of(n_rows - 1)
    gap = max(1, (n_chunks - FREE - primed) // body_units)
    first = min(n_chunks, max(primed, n_chunks - FREE - gap * body_units))
    done = min(body_units, (n_chunks - first) // gap)

    @pl.loop(0, first)
    def _(j):
        step(j)

    @pl.loop(first, n_chunks)
    def _(j):
        step(j)

        u = (j - first) // gap

        @pl.when((lax.rem(j - first, gap) == gap - 1) & (u < done))
        def _():
            compute(u)

    @pl.loop(n_chunks, max(n_chunks, primed + 1))
    def _(j):
        pass_right(j)

    @pl.loop(done, body_units)
    def _(u):
        compute(u)

    def arrived(group, start, size):
        for d in range(1, holders):
            x_arrival(d, group, start, size).wait_recv()

    def half(h, start, cols):
        rights = pl.ds(pl.multiple_of(h * block_cols, block_cols), block_cols)
        return jnp.dot(left[h, start:start + TAIL, :], right[rights, cols], preferred_element_type=jnp.float32)

    tiles = [slice(t, t + TILE) for t in range(0, block_cols, TILE)]
    start = block_rows - GROUP
    arrived(tail_sem, start, TAIL)
    for cols in tiles:
        counts = half(0, start, cols)
        for h in range(1, holders):
            counts += half(h, start, cols)
        out[start:start + TAIL, cols] = jnp.where(
            counts > 0.5, 1, adj[start:start + TAIL, cols]).astype(out.dtype)

    start = block_rows - TAIL
    for cols in tiles:
        partial[:, cols] = half(lo, start, cols) + adj[start:start + TAIL, cols].astype(jnp.float32)

    arrived(tail_sem + 1, start, TAIL - SPLIT)
    for core in cores:
        @pl.when(on_core[core] & (hi == 0))
        def _():
            pl.semaphore_wait(ready, len(spared_by[core]))
            for copy in far_copies(core, early, block_rows - SPLIT):
                copy.start()

    arrived(tail_sem + 2, block_rows - SPLIT, SPLIT)
    for core in cores:
        @pl.when(on_core[core] & (hi == 0))
        def _():
            for copy in far_copies(core, late, block_rows):
                copy.start()

    whole = left.at[lo]

    @pl.when(feeds_next)
    def _():
        pltpu.make_async_remote_copy(
            src_ref=whole, dst_ref=whole, send_sem=z_send, recv_sem=z_recv.at[0],
            device_id={"col": next_col}, device_id_type=MESH).wait_send()

    @pl.when(feeds_back)
    def _():
        pltpu.make_async_remote_copy(
            src_ref=whole, dst_ref=whole, send_sem=b_send, recv_sem=z_recv.at[0],
            device_id={"col": back_col}, device_id_type=MESH).wait_send()

    def x_sent(chunks):
        part = left.at[lo, pl.ds(0, chunks * CHUNK)]
        for d in range(1, holders):
            pltpu.make_async_remote_copy(
                src_ref=part, dst_ref=part, send_sem=x_send.at[d - 1], recv_sem=x_recv.at[d - 1, 0],
                device_id={"col": hi * holders + lax.rem(lo + d, holders)}, device_id_type=MESH).wait_send()

    for chunks in sorted({0, *(early[core].get(stage, 0) + late[core].get(stage, 0) for core in cores for stage in spared_by[core])}):
        @pl.when(spared[0] + spared[1] == chunks)
        def _():
            x_sent(n_chunks - chunks)

    for core in cores:
        @pl.when(on_core[core] & (hi == 0))
        def _():
            for copy in far_copies(core, early, block_rows - SPLIT) + far_copies(core, late, block_rows):
                copy.wait_send()

    @pl.when(r < n_rows - 1)
    def _():
        pltpu.make_async_remote_copy(
            src_ref=right, dst_ref=right, send_sem=r_send, recv_sem=r_recv.at[0],
            device_id={"row": r + 1}, device_id_type=MESH).wait_send()


def finish(closed, left, right, partial, out, tail, sems):
    holders = left.shape[0]
    block_rows, block_cols = closed.shape
    lo = lax.rem(lax.axis_index("col"), holders)
    body = block_rows - TAIL
    bulk = pltpu.make_async_copy(closed.at[0:body], out.at[0:body], sems.at[0])
    bulk.start()
    for t in range(0, block_cols, TILE):
        cols = slice(t, t + TILE)
        counts = partial[:, cols]
        for d in range(1, holders):
            h = lax.rem(lo + holders - d, holders)
            rights = pl.ds(pl.multiple_of(h * block_cols, block_cols), block_cols)
            counts += jnp.dot(left[h, body:block_rows, :], right[rights, cols], preferred_element_type=jnp.float32)
        tail[:, cols] = jnp.where(counts > 0.5, 1, 0).astype(tail.dtype)
    last = pltpu.make_async_copy(tail, out.at[body:block_rows], sems.at[1])
    last.start()
    bulk.wait()
    last.wait()


def per_device(n_rows, n_cols, adjacency):
    block_rows, block_cols = adjacency.shape
    window = PANELS * PANEL
    holders = window // block_cols
    dma = pltpu.SemaphoreType.DMA
    parts = pl.pallas_call(
        functools.partial(kernel, n_rows, n_cols, window),
        out_shape=[
            pltpu.VMEM((block_rows, block_cols), jnp.bfloat16),
            pltpu.VMEM((holders, block_rows, block_cols), jnp.bfloat16),
            pltpu.VMEM((window, block_cols), jnp.bfloat16),
            pltpu.VMEM((TAIL, block_cols), jnp.float32),
        ],
        in_specs=[pl.BlockSpec(memory_space=pltpu.HBM)],
        out_specs=[pl.BlockSpec(memory_space=pltpu.VMEM)] * 4,
        scratch_shapes=[
            pltpu.VMEM((block_rows, block_cols), jnp.int32),
            dma((2,)),
            dma,
            dma,
            dma((RING,)),
            dma((holders - 1,)),
            dma((holders - 1, block_rows // GROUP + 2 - (block_rows // GROUP - 1) // 2)),
            dma,
            dma((RIGHTS,)),
            pltpu.SemaphoreType.REGULAR((3,)),
            dma((holders - 1, max(len(a) + len(b) for a, b in zip(EARLY, LATE)))),
            pltpu.SemaphoreType.REGULAR,
        ],
        compiler_params=pltpu.CompilerParams(
            collective_id=0, has_side_effects=True, vmem_limit_bytes=20 * 1024 * 1024),
    )(pltpu.with_memory_space_constraint(adjacency, pltpu.HBM))
    return pl.pallas_call(
        finish,
        out_shape=jax.ShapeDtypeStruct((block_rows, block_cols), jnp.bfloat16),
        in_specs=[pl.BlockSpec(memory_space=pltpu.VMEM)] * 4,
        out_specs=pl.BlockSpec(memory_space=pltpu.HBM),
        scratch_shapes=[pltpu.VMEM((TAIL, block_cols), jnp.bfloat16), dma((2,))],
        compiler_params=pltpu.CompilerParams(vmem_limit_bytes=8 * 1024 * 1024),
    )(*parts)


def solution(mesh):
    spec = P("row", "col")
    return jax.shard_map(
        functools.partial(per_device, mesh.shape["row"], mesh.shape["col"]),
        mesh=mesh, in_specs=(spec,), out_specs=spec, check_vma=False)
```

```python
import functools

import jax
import jax.numpy as jnp
from jax import lax
from jax.experimental import pallas as pl
from jax.experimental.pallas import tpu as pltpu
from jax.sharding import PartitionSpec as P

PANEL = 512
PANELS = 4

CHUNK = 16
CONVERT = 16
EVERY = CONVERT // CHUNK
FREE = 4
RIGHT = 128
LOAD = 128
FIRST = 128
GROUP = 256
TAIL = 128
SPLIT = 32
TILE = 512
UNIT = 256
RING = 16
CREDIT = 8
RIGHTS = 4
EARLY = ({1: 3}, {})
LATE = ({1: 2, 3: 2}, {1: 1})
PACE = RIGHT // (2 * CHUNK)
MESH = pl.DeviceIdType.MESH


def lag_of(row):
    return PACE * (1 + row) + (3 * PACE // 2) * (row // 2)


def kernel(n_rows, n_cols, window, adj_hbm, out, left, right, partial, adj,
           adj_sem, z_send, b_send, z_recv, x_send, x_recv, r_send, r_recv, credit, f_send, ready):
    block_rows, block_cols = adj.shape
    holders = left.shape[0]
    stages = n_cols // holders
    n_chunks = block_rows // CHUNK
    n_right = window // RIGHT
    n_units = block_cols // UNIT
    tail_from = n_chunks - TAIL // CHUNK
    split_from = n_chunks - SPLIT // CHUNK
    early, late = ([{stage: chunks for stage, chunks in core.items() if stage < n_cols // holders} for core in spare]
                   for spare in (EARLY, LATE))
    spared_by = [sorted({*a, *b}) for a, b in zip(early, late)]
    cores = [core for core in range(2) if spared_by[core]]

    r = lax.axis_index("row")
    c = lax.axis_index("col")
    hi = c // holders
    lo = lax.rem(c, holders)
    lag = lag_of(r)

    relay = lax.rem(hi, 2) == 0
    feeds_next = relay & (hi < stages - 1)
    feeds_back = relay & (hi > 0)
    next_col = c + holders * (1 + (hi + 2 < stages).astype(jnp.int32))
    back_col = c - holders

    source = jnp.where(relay, c - 2 * holders, jnp.where(hi == stages - 1, back_col, c + holders))
    as_next = relay | (hi == stages - 1)
    on_core = [lax.rem(r, 2) == core for core in range(2)]
    spared = [jnp.int32(0)] * 2
    for i, spare in enumerate((early, late)):
        for core in cores:
            for stage, chunks in spare[core].items():
                spared[i] = jnp.where(on_core[core] & (hi == stage), chunks, spared[i])

    def crosses(j):
        return (j < split_from - spared[0]) | ((j >= split_from) & (j < n_chunks - spared[1]))

    def load(start, size, sem):
        rows = pl.ds(pl.multiple_of(start, CONVERT), size)
        return pltpu.make_async_copy(adj_hbm.at[rows], adj.at[rows], adj_sem.at[sem])

    head = load(0, FIRST, 0)
    rest = load(FIRST, block_rows - FIRST, 1)

    def chunk(j):
        return pl.ds(pl.multiple_of(j * CHUNK, CHUNK), CHUNK)

    def z_copy(j):
        part = left.at[lo, chunk(j)]
        return pltpu.make_async_remote_copy(
            src_ref=part, dst_ref=part, send_sem=z_send, recv_sem=z_recv.at[lax.rem(j, RING)],
            device_id={"col": next_col}, device_id_type=MESH)

    def z_back(j):
        part = left.at[lo, chunk(j)]
        return pltpu.make_async_remote_copy(
            src_ref=part, dst_ref=part, send_sem=b_send, recv_sem=z_recv.at[lax.rem(j, RING)],
            device_id={"col": back_col}, device_id_type=MESH)

    def x_group(j):
        return j // (GROUP // CHUNK) + (j >= tail_from).astype(jnp.int32) + (j >= split_from).astype(jnp.int32)

    def x_copy(d, j):
        part = left.at[lo, chunk(j)]
        peer = hi * holders + lax.rem(lo + d, holders)
        return pltpu.make_async_remote_copy(
            src_ref=part, dst_ref=part, send_sem=x_send.at[d - 1], recv_sem=x_recv.at[d - 1, x_group(j)],
            device_id={"col": peer}, device_id_type=MESH)

    def x_arrival(d, group, start, size):
        part = left.at[lax.rem(lo + holders - d, holders), pl.ds(pl.multiple_of(start, CHUNK), size)]
        peer = hi * holders + lax.rem(lo + holders - d, holders)
        return pltpu.make_async_remote_copy(
            src_ref=part, dst_ref=part, send_sem=x_send.at[d - 1], recv_sem=x_recv.at[d - 1, group],
            device_id={"col": peer}, device_id_type=MESH)

    def far_copy(d, stage, chunks, end, sem):
        rows = chunks * CHUNK
        part = left.at[lax.rem(lo + holders - d, holders), pl.ds(end - rows, rows)]
        return pltpu.make_async_remote_copy(
            src_ref=part, dst_ref=part, send_sem=f_send.at[d - 1, sem],
            recv_sem=x_recv.at[d - 1, block_rows // GROUP + (end == block_rows)],
            device_id={"col": stage * holders + lo}, device_id_type=MESH)

    def far_copies(core, spare, end):
        first_sem = len(early[core]) if end == block_rows else 0
        return [far_copy(d, stage, spare[core][stage], end, first_sem + i)
                for i, stage in enumerate(sorted(spare[core], reverse=True)) for d in range(1, holders)]

    def r_rows(i):
        return pl.ds(pl.multiple_of(i * RIGHT, RIGHT), RIGHT)

    def r_copy(i):
        part = right.at[r_rows(i)]
        return pltpu.make_async_remote_copy(
            src_ref=part, dst_ref=part, send_sem=r_send, recv_sem=r_recv.at[lax.rem(i, RIGHTS)],
            device_id={"row": r + 1}, device_id_type=MESH)

    head.start()

    barrier = pltpu.get_barrier_semaphore()

    def greet(where):
        pl.semaphore_signal(barrier, inc=1, device_id=where, device_id_type=MESH)

    @pl.when(feeds_back)
    def _():
        greet({"col": c - 2 * holders})
        greet({"col": back_col})

    @pl.when(feeds_next)
    def _():
        greet({"col": next_col})

    @pl.when(~relay & (hi < stages - 1))
    def _():
        greet({"col": c + holders})

    @pl.when(~relay & (hi == stages - 1))
    def _():
        greet({"col": c - holders})

    for d in range(1, holders):
        greet({"col": hi * holders + lax.rem(lo + d, holders)})

    for core in cores:
        @pl.when(on_core[core] & (hi == 0))
        def _():
            for stage in spared_by[core]:
                greet({"col": stage * holders + lo})

    @pl.when(r > 0)
    def _():
        greet({"row": r - 1})

    @pl.when(r < n_rows - 1)
    def _():
        greet({"row": r + 1})

    def convert_left(i):
        rows = pl.ds(pl.multiple_of(i * CONVERT, CONVERT), CONVERT)
        left[lo, rows, :] = adj[rows, :].astype(jnp.bfloat16)

    def convert_right(i):
        right[r_rows(i), :] = adj[r_rows(i), :].astype(jnp.bfloat16)

    ahead = FIRST // CONVERT
    behind = ahead // 2

    @pl.loop(FIRST // LOAD, block_rows // LOAD)
    def _(i):
        load(i * LOAD, LOAD, 1).start()

    head.wait()

    @pl.when(hi == 0)
    def _():
        for k in range(ahead):
            convert_left(k)

    known = (2 * feeds_back.astype(jnp.int32) + feeds_next.astype(jnp.int32)
             + (~relay).astype(jnp.int32) + (holders - 1)
             + (r > 0).astype(jnp.int32) + (r < n_rows - 1).astype(jnp.int32))
    spared_here = [on_core[core] & (hi == stage) for core in cores for stage in spared_by[core]]
    for here in spared_here:
        known += here.astype(jnp.int32)
    pl.semaphore_wait(barrier, known)

    for here in spared_here:
        @pl.when(here)
        def _():
            pl.semaphore_signal(ready, inc=1, device_id={"col": lo}, device_id_type=MESH)

    def paid(j):
        return (lax.rem(j, CREDIT) == 0) & (j >= RING)

    def pass_right(j):
        late = j - lag
        i = late // PACE

        @pl.when((late >= 0) & (lax.rem(late, PACE) == 0) & (i < n_right))
        def _():
            @pl.when(r > 0)
            def _():
                r_copy(i).wait_recv()

                @pl.when(i < n_right - RIGHTS)
                def _():
                    pl.semaphore_signal(credit.at[2], inc=1, device_id={"row": r - 1}, device_id_type=MESH)

            @pl.when(r < n_rows - 1)
            def _():
                @pl.when(i >= RIGHTS)
                def _():
                    pl.semaphore_wait(credit.at[2], 1)

                r_copy(i).start()

    def step(j):
        @pl.when(hi > 0)
        def _():
            z_copy(j).wait_recv()

        @pl.when(feeds_next)
        def _():
            @pl.when(paid(j))
            def _():
                pl.semaphore_wait(credit.at[0], 1)

            z_copy(j).start()

        @pl.when(feeds_back)
        def _():
            @pl.when(paid(j))
            def _():
                pl.semaphore_wait(credit.at[1], 1)

            z_back(j).start()

        @pl.when(crosses(j))
        def _():
            for d in range(1, holders):
                x_copy(d, j).start()

        @pl.when((hi > 0) & (lax.rem(j + 1, CREDIT) == 0) & (j + 1 <= n_chunks - RING))
        def _():
            pl.semaphore_signal(credit.at[jnp.where(as_next, 0, 1)], inc=1,
                                device_id={"col": source}, device_id_type=MESH)

        pass_right(j)

        @pl.when(j == EVERY * behind)
        def _():
            rest.wait()

        unit = j // EVERY + ahead - behind

        @pl.when((hi == 0) & (lax.rem(j, EVERY) == 0) & (unit >= ahead) & (unit < block_rows // CONVERT))
        def _():
            convert_left(unit)

        @pl.when((r == 0) & (lax.rem(j, PACE) == 0) & (j < PACE * n_right))
        def _():
            convert_right(j // PACE)

    def compute(u):
        g = u // n_units
        t = lax.rem(u, n_units)

        @pl.when(t == 0)
        def _():
            for d in range(1, holders):
                x_arrival(d, g, g * GROUP, GROUP).wait_recv()

        rows = pl.ds(pl.multiple_of(g * GROUP, GROUP), GROUP)
        cols = pl.ds(pl.multiple_of(t * UNIT, UNIT), UNIT)
        counts = jnp.zeros((GROUP, UNIT), jnp.float32)
        for h in range(holders):
            counts += jnp.dot(left[h, rows, :], right[h * block_cols:(h + 1) * block_cols, cols],
                              preferred_element_type=jnp.float32)
        out[rows, cols] = jnp.where(counts > 0.5, 1, adj[rows, cols]).astype(out.dtype)

    body_units = (block_rows // GROUP - 1) * n_units
    primed = PACE * (n_right - 1) + lag_of(n_rows - 1)
    gap = max(1, (n_chunks - FREE - primed) // body_units)
    first = min(n_chunks, max(primed, n_chunks - FREE - gap * body_units))
    done = min(body_units, (n_chunks - first) // gap)

    @pl.loop(0, first)
    def _(j):
        step(j)

    @pl.loop(first, n_chunks)
    def _(j):
        step(j)

        u = (j - first) // gap

        @pl.when((lax.rem(j - first, gap) == gap - 1) & (u < done))
        def _():
            compute(u)

    @pl.loop(n_chunks, max(n_chunks, primed + 1))
    def _(j):
        pass_right(j)

    @pl.loop(done, body_units)
    def _(u):
        compute(u)

    def arrived(group, start, size):
        for d in range(1, holders):
            x_arrival(d, group, start, size).wait_recv()

    def half(h, start, cols):
        rights = pl.ds(pl.multiple_of(h * block_cols, block_cols), block_cols)
        return jnp.dot(left[h, start:start + TAIL, :], right[rights, cols], preferred_element_type=jnp.float32)

    tiles = [slice(t, t + TILE) for t in range(0, block_cols, TILE)]
    start = block_rows - GROUP
    arrived(block_rows // GROUP - 1, start, TAIL)
    for cols in tiles:
        counts = half(0, start, cols)
        for h in range(1, holders):
            counts += half(h, start, cols)
        out[start:start + TAIL, cols] = jnp.where(
            counts > 0.5, 1, adj[start:start + TAIL, cols]).astype(out.dtype)

    start = block_rows - TAIL
    for cols in tiles:
        partial[:, cols] = half(lo, start, cols) + adj[start:start + TAIL, cols].astype(jnp.float32)

    arrived(block_rows // GROUP, start, TAIL - SPLIT)
    for core in cores:
        @pl.when(on_core[core] & (hi == 0))
        def _():
            pl.semaphore_wait(ready, len(spared_by[core]))
            for copy in far_copies(core, early, block_rows - SPLIT):
                copy.start()

    arrived(block_rows // GROUP + 1, block_rows - SPLIT, SPLIT)
    for core in cores:
        @pl.when(on_core[core] & (hi == 0))
        def _():
            for copy in far_copies(core, late, block_rows):
                copy.start()

    whole = left.at[lo]

    @pl.when(feeds_next)
    def _():
        pltpu.make_async_remote_copy(
            src_ref=whole, dst_ref=whole, send_sem=z_send, recv_sem=z_recv.at[0],
            device_id={"col": next_col}, device_id_type=MESH).wait_send()

    @pl.when(feeds_back)
    def _():
        pltpu.make_async_remote_copy(
            src_ref=whole, dst_ref=whole, send_sem=b_send, recv_sem=z_recv.at[0],
            device_id={"col": back_col}, device_id_type=MESH).wait_send()

    def x_sent(chunks):
        part = left.at[lo, pl.ds(0, chunks * CHUNK)]
        for d in range(1, holders):
            pltpu.make_async_remote_copy(
                src_ref=part, dst_ref=part, send_sem=x_send.at[d - 1], recv_sem=x_recv.at[d - 1, 0],
                device_id={"col": hi * holders + lax.rem(lo + d, holders)}, device_id_type=MESH).wait_send()

    for chunks in sorted({0, *(early[core].get(stage, 0) + late[core].get(stage, 0) for core in cores for stage in spared_by[core])}):
        @pl.when(spared[0] + spared[1] == chunks)
        def _():
            x_sent(n_chunks - chunks)

    for core in cores:
        @pl.when(on_core[core] & (hi == 0))
        def _():
            for copy in far_copies(core, early, block_rows - SPLIT) + far_copies(core, late, block_rows):
                copy.wait_send()

    @pl.when(r < n_rows - 1)
    def _():
        pltpu.make_async_remote_copy(
            src_ref=right, dst_ref=right, send_sem=r_send, recv_sem=r_recv.at[0],
            device_id={"row": r + 1}, device_id_type=MESH).wait_send()


def finish(closed, left, right, partial, out, tail, sems):
    holders = left.shape[0]
    block_rows, block_cols = closed.shape
    lo = lax.rem(lax.axis_index("col"), holders)
    body = block_rows - TAIL
    bulk = pltpu.make_async_copy(closed.at[0:body], out.at[0:body], sems.at[0])
    bulk.start()
    for t in range(0, block_cols, TILE):
        cols = slice(t, t + TILE)
        counts = partial[:, cols]
        for d in range(1, holders):
            h = lax.rem(lo + holders - d, holders)
            rights = pl.ds(pl.multiple_of(h * block_cols, block_cols), block_cols)
            counts += jnp.dot(left[h, body:block_rows, :], right[rights, cols], preferred_element_type=jnp.float32)
        tail[:, cols] = jnp.where(counts > 0.5, 1, 0).astype(tail.dtype)
    last = pltpu.make_async_copy(tail, out.at[body:block_rows], sems.at[1])
    last.start()
    bulk.wait()
    last.wait()


def per_device(n_rows, n_cols, adjacency):
    block_rows, block_cols = adjacency.shape
    window = PANELS * PANEL
    holders = window // block_cols
    dma = pltpu.SemaphoreType.DMA
    parts = pl.pallas_call(
        functools.partial(kernel, n_rows, n_cols, window),
        out_shape=[
            pltpu.VMEM((block_rows, block_cols), jnp.bfloat16),
            pltpu.VMEM((holders, block_rows, block_cols), jnp.bfloat16),
            pltpu.VMEM((window, block_cols), jnp.bfloat16),
            pltpu.VMEM((TAIL, block_cols), jnp.float32),
        ],
        in_specs=[pl.BlockSpec(memory_space=pltpu.HBM)],
        out_specs=[pl.BlockSpec(memory_space=pltpu.VMEM)] * 4,
        scratch_shapes=[
            pltpu.VMEM((block_rows, block_cols), jnp.int32),
            dma((2,)),
            dma,
            dma,
            dma((RING,)),
            dma((holders - 1,)),
            dma((holders - 1, block_rows // GROUP + 2)),
            dma,
            dma((RIGHTS,)),
            pltpu.SemaphoreType.REGULAR((3,)),
            dma((holders - 1, max(len(a) + len(b) for a, b in zip(EARLY, LATE)))),
            pltpu.SemaphoreType.REGULAR,
        ],
        compiler_params=pltpu.CompilerParams(
            collective_id=0, has_side_effects=True, vmem_limit_bytes=20 * 1024 * 1024),
    )(pltpu.with_memory_space_constraint(adjacency, pltpu.HBM))
    return pl.pallas_call(
        finish,
        out_shape=jax.ShapeDtypeStruct((block_rows, block_cols), jnp.bfloat16),
        in_specs=[pl.BlockSpec(memory_space=pltpu.VMEM)] * 4,
        out_specs=pl.BlockSpec(memory_space=pltpu.HBM),
        scratch_shapes=[pltpu.VMEM((TAIL, block_cols), jnp.bfloat16), dma((2,))],
        compiler_params=pltpu.CompilerParams(vmem_limit_bytes=8 * 1024 * 1024),
    )(*parts)


def solution(mesh):
    spec = P("row", "col")
    return jax.shard_map(
        functools.partial(per_device, mesh.shape["row"], mesh.shape["col"]),
        mesh=mesh, in_specs=(spec,), out_specs=spec, check_vma=False)
```

```python
import functools

import jax
import jax.numpy as jnp
from jax import lax
from jax.experimental import pallas as pl
from jax.experimental.pallas import tpu as pltpu
from jax.sharding import PartitionSpec as P

PANEL = 512
PANELS = 4

CHUNK = 8
CONVERT = 16
EVERY = CONVERT // CHUNK
FREE = 8
RIGHT = 128
LOAD = 128
FIRST = 128
GROUP = 256
TAIL = 128
SPLIT = 32
TILE = 512
UNIT = 256
RING = 32
CREDIT = 16
RIGHTS = 4
EARLY = ({1: 4}, {})
LATE = ({1: 4, 3: 4}, {1: 2})
PACE = RIGHT // (2 * CHUNK)
MESH = pl.DeviceIdType.MESH


def lag_of(row):
    return PACE * (1 + row) + (3 * PACE // 2) * (row // 2)


def kernel(n_rows, n_cols, window, adj_hbm, out, left, right, partial, adj,
           adj_sem, z_send, b_send, z_recv, x_send, x_recv, r_send, r_recv, credit, f_send, ready):
    block_rows, block_cols = adj.shape
    holders = left.shape[0]
    stages = n_cols // holders
    n_chunks = block_rows // CHUNK
    n_right = window // RIGHT
    n_units = block_cols // UNIT
    tail_from = n_chunks - TAIL // CHUNK
    split_from = n_chunks - SPLIT // CHUNK
    early, late = ([{stage: chunks for stage, chunks in core.items() if stage < n_cols // holders} for core in spare]
                   for spare in (EARLY, LATE))
    spared_by = [sorted({*a, *b}) for a, b in zip(early, late)]
    cores = [core for core in range(2) if spared_by[core]]

    r = lax.axis_index("row")
    c = lax.axis_index("col")
    hi = c // holders
    lo = lax.rem(c, holders)
    lag = lag_of(r)

    relay = lax.rem(hi, 2) == 0
    feeds_next = relay & (hi < stages - 1)
    feeds_back = relay & (hi > 0)
    next_col = c + holders * (1 + (hi + 2 < stages).astype(jnp.int32))
    back_col = c - holders

    source = jnp.where(relay, c - 2 * holders, jnp.where(hi == stages - 1, back_col, c + holders))
    as_next = relay | (hi == stages - 1)
    on_core = [lax.rem(r, 2) == core for core in range(2)]
    spared = [jnp.int32(0)] * 2
    for i, spare in enumerate((early, late)):
        for core in cores:
            for stage, chunks in spare[core].items():
                spared[i] = jnp.where(on_core[core] & (hi == stage), chunks, spared[i])

    def crosses(j):
        return (j < split_from - spared[0]) | ((j >= split_from) & (j < n_chunks - spared[1]))

    def load(start, size, sem):
        rows = pl.ds(pl.multiple_of(start, CONVERT), size)
        return pltpu.make_async_copy(adj_hbm.at[rows], adj.at[rows], adj_sem.at[sem])

    head = load(0, FIRST, 0)
    rest = load(FIRST, block_rows - FIRST, 1)

    def chunk(j):
        return pl.ds(pl.multiple_of(j * CHUNK, CHUNK), CHUNK)

    def z_copy(j):
        part = left.at[lo, chunk(j)]
        return pltpu.make_async_remote_copy(
            src_ref=part, dst_ref=part, send_sem=z_send, recv_sem=z_recv.at[lax.rem(j, RING)],
            device_id={"col": next_col}, device_id_type=MESH)

    def z_back(j):
        part = left.at[lo, chunk(j)]
        return pltpu.make_async_remote_copy(
            src_ref=part, dst_ref=part, send_sem=b_send, recv_sem=z_recv.at[lax.rem(j, RING)],
            device_id={"col": back_col}, device_id_type=MESH)

    def x_group(j):
        return j // (GROUP // CHUNK) + (j >= tail_from).astype(jnp.int32) + (j >= split_from).astype(jnp.int32)

    def x_copy(d, j):
        part = left.at[lo, chunk(j)]
        peer = hi * holders + lax.rem(lo + d, holders)
        return pltpu.make_async_remote_copy(
            src_ref=part, dst_ref=part, send_sem=x_send.at[d - 1], recv_sem=x_recv.at[d - 1, x_group(j)],
            device_id={"col": peer}, device_id_type=MESH)

    def x_arrival(d, group, start, size):
        part = left.at[lax.rem(lo + holders - d, holders), pl.ds(pl.multiple_of(start, CHUNK), size)]
        peer = hi * holders + lax.rem(lo + holders - d, holders)
        return pltpu.make_async_remote_copy(
            src_ref=part, dst_ref=part, send_sem=x_send.at[d - 1], recv_sem=x_recv.at[d - 1, group],
            device_id={"col": peer}, device_id_type=MESH)

    def far_copy(d, stage, chunks, end, sem):
        rows = chunks * CHUNK
        part = left.at[lax.rem(lo + holders - d, holders), pl.ds(end - rows, rows)]
        return pltpu.make_async_remote_copy(
            src_ref=part, dst_ref=part, send_sem=f_send.at[d - 1, sem],
            recv_sem=x_recv.at[d - 1, block_rows // GROUP + (end == block_rows)],
            device_id={"col": stage * holders + lo}, device_id_type=MESH)

    def far_copies(core, spare, end):
        first_sem = len(early[core]) if end == block_rows else 0
        return [far_copy(d, stage, spare[core][stage], end, first_sem + i)
                for i, stage in enumerate(sorted(spare[core], reverse=True)) for d in range(1, holders)]

    def r_rows(i):
        return pl.ds(pl.multiple_of(i * RIGHT, RIGHT), RIGHT)

    def r_copy(i):
        part = right.at[r_rows(i)]
        return pltpu.make_async_remote_copy(
            src_ref=part, dst_ref=part, send_sem=r_send, recv_sem=r_recv.at[lax.rem(i, RIGHTS)],
            device_id={"row": r + 1}, device_id_type=MESH)

    head.start()

    barrier = pltpu.get_barrier_semaphore()

    def greet(where):
        pl.semaphore_signal(barrier, inc=1, device_id=where, device_id_type=MESH)

    @pl.when(feeds_back)
    def _():
        greet({"col": c - 2 * holders})
        greet({"col": back_col})

    @pl.when(feeds_next)
    def _():
        greet({"col": next_col})

    @pl.when(~relay & (hi < stages - 1))
    def _():
        greet({"col": c + holders})

    @pl.when(~relay & (hi == stages - 1))
    def _():
        greet({"col": c - holders})

    for d in range(1, holders):
        greet({"col": hi * holders + lax.rem(lo + d, holders)})

    for core in cores:
        @pl.when(on_core[core] & (hi == 0))
        def _():
            for stage in spared_by[core]:
                greet({"col": stage * holders + lo})

    @pl.when(r > 0)
    def _():
        greet({"row": r - 1})

    @pl.when(r < n_rows - 1)
    def _():
        greet({"row": r + 1})

    def convert_left(i):
        rows = pl.ds(pl.multiple_of(i * CONVERT, CONVERT), CONVERT)
        left[lo, rows, :] = adj[rows, :].astype(jnp.bfloat16)

    def convert_right(i):
        right[r_rows(i), :] = adj[r_rows(i), :].astype(jnp.bfloat16)

    ahead = FIRST // CONVERT
    behind = ahead // 2

    @pl.loop(FIRST // LOAD, block_rows // LOAD)
    def _(i):
        load(i * LOAD, LOAD, 1).start()

    head.wait()

    @pl.when(hi == 0)
    def _():
        for k in range(ahead):
            convert_left(k)

    known = (2 * feeds_back.astype(jnp.int32) + feeds_next.astype(jnp.int32)
             + (~relay).astype(jnp.int32) + (holders - 1)
             + (r > 0).astype(jnp.int32) + (r < n_rows - 1).astype(jnp.int32))
    spared_here = [on_core[core] & (hi == stage) for core in cores for stage in spared_by[core]]
    for here in spared_here:
        known += here.astype(jnp.int32)
    pl.semaphore_wait(barrier, known)

    for here in spared_here:
        @pl.when(here)
        def _():
            pl.semaphore_signal(ready, inc=1, device_id={"col": lo}, device_id_type=MESH)

    def paid(j):
        return (lax.rem(j, CREDIT) == 0) & (j >= RING)

    def pass_right(j):
        late = j - lag
        i = late // PACE

        @pl.when((late >= 0) & (lax.rem(late, PACE) == 0) & (i < n_right))
        def _():
            @pl.when(r > 0)
            def _():
                r_copy(i).wait_recv()

                @pl.when(i < n_right - RIGHTS)
                def _():
                    pl.semaphore_signal(credit.at[2], inc=1, device_id={"row": r - 1}, device_id_type=MESH)

            @pl.when(r < n_rows - 1)
            def _():
                @pl.when(i >= RIGHTS)
                def _():
                    pl.semaphore_wait(credit.at[2], 1)

                r_copy(i).start()

    def step(j):
        @pl.when(hi > 0)
        def _():
            z_copy(j).wait_recv()

        @pl.when(feeds_next)
        def _():
            @pl.when(paid(j))
            def _():
                pl.semaphore_wait(credit.at[0], 1)

            z_copy(j).start()

        @pl.when(feeds_back)
        def _():
            @pl.when(paid(j))
            def _():
                pl.semaphore_wait(credit.at[1], 1)

            z_back(j).start()

        @pl.when(crosses(j))
        def _():
            for d in range(1, holders):
                x_copy(d, j).start()

        @pl.when((hi > 0) & (lax.rem(j + 1, CREDIT) == 0) & (j + 1 <= n_chunks - RING))
        def _():
            pl.semaphore_signal(credit.at[jnp.where(as_next, 0, 1)], inc=1,
                                device_id={"col": source}, device_id_type=MESH)

        pass_right(j)

        @pl.when(j == EVERY * behind)
        def _():
            rest.wait()

        unit = j // EVERY + ahead - behind

        @pl.when((hi == 0) & (lax.rem(j, EVERY) == 0) & (unit >= ahead) & (unit < block_rows // CONVERT))
        def _():
            convert_left(unit)

        @pl.when((r == 0) & (lax.rem(j, PACE) == 0) & (j < PACE * n_right))
        def _():
            convert_right(j // PACE)

    def compute(u):
        g = u // n_units
        t = lax.rem(u, n_units)

        @pl.when(t == 0)
        def _():
            for d in range(1, holders):
                x_arrival(d, g, g * GROUP, GROUP).wait_recv()

        rows = pl.ds(pl.multiple_of(g * GROUP, GROUP), GROUP)
        cols = pl.ds(pl.multiple_of(t * UNIT, UNIT), UNIT)
        counts = jnp.zeros((GROUP, UNIT), jnp.float32)
        for h in range(holders):
            counts += jnp.dot(left[h, rows, :], right[h * block_cols:(h + 1) * block_cols, cols],
                              preferred_element_type=jnp.float32)
        out[rows, cols] = jnp.where(counts > 0.5, 1, adj[rows, cols]).astype(out.dtype)

    body_units = (block_rows // GROUP - 1) * n_units
    primed = PACE * (n_right - 1) + lag_of(n_rows - 1)
    gap = max(1, (n_chunks - FREE - primed) // body_units)
    first = min(n_chunks, max(primed, n_chunks - FREE - gap * body_units))
    done = min(body_units, (n_chunks - first) // gap)

    @pl.loop(0, first)
    def _(j):
        step(j)

    @pl.loop(first, n_chunks)
    def _(j):
        step(j)

        u = (j - first) // gap

        @pl.when((lax.rem(j - first, gap) == gap - 1) & (u < done))
        def _():
            compute(u)

    @pl.loop(n_chunks, max(n_chunks, primed + 1))
    def _(j):
        pass_right(j)

    @pl.loop(done, body_units)
    def _(u):
        compute(u)

    def arrived(group, start, size):
        for d in range(1, holders):
            x_arrival(d, group, start, size).wait_recv()

    def half(h, start, cols):
        rights = pl.ds(pl.multiple_of(h * block_cols, block_cols), block_cols)
        return jnp.dot(left[h, start:start + TAIL, :], right[rights, cols], preferred_element_type=jnp.float32)

    tiles = [slice(t, t + TILE) for t in range(0, block_cols, TILE)]
    start = block_rows - GROUP
    arrived(block_rows // GROUP - 1, start, TAIL)
    for cols in tiles:
        counts = half(0, start, cols)
        for h in range(1, holders):
            counts += half(h, start, cols)
        out[start:start + TAIL, cols] = jnp.where(
            counts > 0.5, 1, adj[start:start + TAIL, cols]).astype(out.dtype)

    start = block_rows - TAIL
    for cols in tiles:
        partial[:, cols] = half(lo, start, cols) + adj[start:start + TAIL, cols].astype(jnp.float32)

    arrived(block_rows // GROUP, start, TAIL - SPLIT)
    for core in cores:
        @pl.when(on_core[core] & (hi == 0))
        def _():
            pl.semaphore_wait(ready, len(spared_by[core]))
            for copy in far_copies(core, early, block_rows - SPLIT):
                copy.start()

    arrived(block_rows // GROUP + 1, block_rows - SPLIT, SPLIT)
    for core in cores:
        @pl.when(on_core[core] & (hi == 0))
        def _():
            for copy in far_copies(core, late, block_rows):
                copy.start()

    whole = left.at[lo]

    @pl.when(feeds_next)
    def _():
        pltpu.make_async_remote_copy(
            src_ref=whole, dst_ref=whole, send_sem=z_send, recv_sem=z_recv.at[0],
            device_id={"col": next_col}, device_id_type=MESH).wait_send()

    @pl.when(feeds_back)
    def _():
        pltpu.make_async_remote_copy(
            src_ref=whole, dst_ref=whole, send_sem=b_send, recv_sem=z_recv.at[0],
            device_id={"col": back_col}, device_id_type=MESH).wait_send()

    def x_sent(chunks):
        part = left.at[lo, pl.ds(0, chunks * CHUNK)]
        for d in range(1, holders):
            pltpu.make_async_remote_copy(
                src_ref=part, dst_ref=part, send_sem=x_send.at[d - 1], recv_sem=x_recv.at[d - 1, 0],
                device_id={"col": hi * holders + lax.rem(lo + d, holders)}, device_id_type=MESH).wait_send()

    for chunks in sorted({0, *(early[core].get(stage, 0) + late[core].get(stage, 0) for core in cores for stage in spared_by[core])}):
        @pl.when(spared[0] + spared[1] == chunks)
        def _():
            x_sent(n_chunks - chunks)

    for core in cores:
        @pl.when(on_core[core] & (hi == 0))
        def _():
            for copy in far_copies(core, early, block_rows - SPLIT) + far_copies(core, late, block_rows):
                copy.wait_send()

    @pl.when(r < n_rows - 1)
    def _():
        pltpu.make_async_remote_copy(
            src_ref=right, dst_ref=right, send_sem=r_send, recv_sem=r_recv.at[0],
            device_id={"row": r + 1}, device_id_type=MESH).wait_send()


def finish(closed, left, right, partial, out, tail, sems):
    holders = left.shape[0]
    block_rows, block_cols = closed.shape
    lo = lax.rem(lax.axis_index("col"), holders)
    body = block_rows - TAIL
    bulk = pltpu.make_async_copy(closed.at[0:body], out.at[0:body], sems.at[0])
    bulk.start()
    for t in range(0, block_cols, TILE):
        cols = slice(t, t + TILE)
        counts = partial[:, cols]
        for d in range(1, holders):
            h = lax.rem(lo + holders - d, holders)
            rights = pl.ds(pl.multiple_of(h * block_cols, block_cols), block_cols)
            counts += jnp.dot(left[h, body:block_rows, :], right[rights, cols], preferred_element_type=jnp.float32)
        tail[:, cols] = jnp.where(counts > 0.5, 1, 0).astype(tail.dtype)
    last = pltpu.make_async_copy(tail, out.at[body:block_rows], sems.at[1])
    last.start()
    bulk.wait()
    last.wait()


def per_device(n_rows, n_cols, adjacency):
    block_rows, block_cols = adjacency.shape
    window = PANELS * PANEL
    holders = window // block_cols
    dma = pltpu.SemaphoreType.DMA
    parts = pl.pallas_call(
        functools.partial(kernel, n_rows, n_cols, window),
        out_shape=[
            pltpu.VMEM((block_rows, block_cols), jnp.bfloat16),
            pltpu.VMEM((holders, block_rows, block_cols), jnp.bfloat16),
            pltpu.VMEM((window, block_cols), jnp.bfloat16),
            pltpu.VMEM((TAIL, block_cols), jnp.float32),
        ],
        in_specs=[pl.BlockSpec(memory_space=pltpu.HBM)],
        out_specs=[pl.BlockSpec(memory_space=pltpu.VMEM)] * 4,
        scratch_shapes=[
            pltpu.VMEM((block_rows, block_cols), jnp.int32),
            dma((2,)),
            dma,
            dma,
            dma((RING,)),
            dma((holders - 1,)),
            dma((holders - 1, block_rows // GROUP + 2)),
            dma,
            dma((RIGHTS,)),
            pltpu.SemaphoreType.REGULAR((3,)),
            dma((holders - 1, max(len(a) + len(b) for a, b in zip(EARLY, LATE)))),
            pltpu.SemaphoreType.REGULAR,
        ],
        compiler_params=pltpu.CompilerParams(
            collective_id=0, has_side_effects=True, vmem_limit_bytes=20 * 1024 * 1024),
    )(pltpu.with_memory_space_constraint(adjacency, pltpu.HBM))
    return pl.pallas_call(
        finish,
        out_shape=jax.ShapeDtypeStruct((block_rows, block_cols), jnp.bfloat16),
        in_specs=[pl.BlockSpec(memory_space=pltpu.VMEM)] * 4,
        out_specs=pl.BlockSpec(memory_space=pltpu.HBM),
        scratch_shapes=[pltpu.VMEM((TAIL, block_cols), jnp.bfloat16), dma((2,))],
        compiler_params=pltpu.CompilerParams(vmem_limit_bytes=8 * 1024 * 1024),
    )(*parts)


def solution(mesh):
    spec = P("row", "col")
    return jax.shard_map(
        functools.partial(per_device, mesh.shape["row"], mesh.shape["col"]),
        mesh=mesh, in_specs=(spec,), out_specs=spec, check_vma=False)
```
